32 devices in a mesh: dp: 4 (over y, core), head: 2 (over x), kv: 4 (over z).
Axes of the slice: x: 2, y: 2, z: 4, core: 2. Of those that a mesh axis runs over, the one named last changes fastest.
Arguments:
- teacher_query: bfloat16 [4, 1024, 3584], P('dp', 'kv', 'head'), may hold values from -96 to 96
- teacher_key: bfloat16 [4, 1024, 512], P('dp', 'kv', 'head'), may hold values from -8 to 8
- student_query: bfloat16 [4, 1024, 1792], P('dp', 'kv', 'head'), may hold values from -96 to 96
- student_key: bfloat16 [4, 1024, 256], P('dp', 'kv', 'head'), may hold values from -8 to 8
- pair_table: int32 [14, 2], replicated, may hold values from 0 to 27, as said below
Outputs:
- kl: float32 [4, 14, 1024], P('dp', 'head', 'kv')
- head_loss: float32 [14], P('head')
The draws below stay inside these ranges and needn't reach their ends.
Inputs may be any that keep to these rules, and one draw needn't show every extreme that they name: `pair_table`: each of the 28 teacher heads appears exactly once in the table.
All inputs are finite; a program needn't handle non-finite values.
Results may differ from the reference program's by a relative error of at most 0.0003.
Values may be sent and summed in bfloat16 or wider, within the bound.
A program may use at most 64 MiB of HBM per device.

```python
import math
import jax
import jax.numpy as jnp
from jax import lax

HT = 28
KVT = 4
DH = 128
HS = 14
KVS = 2
L = 1024
SEQS = 4


def key_field(key, heads):
    shape = (SEQS, L, heads, DH)
    row_scale = jnp.exp(jax.random.uniform(jax.random.fold_in(key, 1), (SEQS, L, heads, 1), jnp.float32, math.log(0.5), math.log(2.0)))
    base = jnp.clip(jax.random.normal(key, shape, jnp.float32), -4.0, 4.0)
    return base * row_scale


def query_field(key, heads):
    shape = (SEQS, L, heads, DH)
    row_scale = jnp.exp(jax.random.uniform(jax.random.fold_in(key, 1), (SEQS, L, heads, 1), jnp.float32, math.log(0.3), math.log(3.0)))
    return jnp.clip(jax.random.normal(key, shape, jnp.float32), -5.0, 5.0) * row_scale


def draw_teacher_key(key, part):
    keys = key_field(jax.random.fold_in(key, 11), KVT)
    return keys.reshape(SEQS, L, KVT * DH).astype(jnp.bfloat16)


def draw_student_key(key, part):
    keys = key_field(jax.random.fold_in(key, 12), KVS)
    return keys.reshape(SEQS, L, KVS * DH).astype(jnp.bfloat16)


def draw_teacher_query(key, part):
    queries = query_field(jax.random.fold_in(key, 13), HT)
    return queries.reshape(SEQS, L, HT * DH).astype(jnp.bfloat16)


def draw_student_query(key, part):
    queries = query_field(jax.random.fold_in(key, 14), HS)
    return queries.reshape(SEQS, L, HS * DH).astype(jnp.bfloat16)


def draw_pair_table(key, part):
    order = jax.random.permutation(jax.random.fold_in(key, 15), HT)
    return order.astype(jnp.int32).reshape(HS, 2)


def setup_inputs(seed: int = 0) -> dict:
    streams_of = jax.random.split(jax.random.key(seed), 6)
    teacher_query = draw_teacher_query(jax.random.fold_in(streams_of[5], 71), 0)
    teacher_key = draw_teacher_key(jax.random.fold_in(streams_of[5], 71), 0)
    student_query = draw_student_query(jax.random.fold_in(streams_of[5], 71), 0)
    student_key = draw_student_key(jax.random.fold_in(streams_of[5], 71), 0)
    pair_table = draw_pair_table(jax.random.fold_in(streams_of[5], 71), 0)
    return dict(teacher_query=teacher_query, teacher_key=teacher_key, student_query=student_query, student_key=student_key, pair_table=pair_table)


masked_value = -1e+30

def masked_logits(query_rows, key_rows, causal_mask):
    scale = 1.0 / math.sqrt(DH)
    product = jnp.dot(query_rows.astype(jnp.float32), key_rows.astype(jnp.float32).T, precision=lax.Precision.HIGHEST, preferred_element_type=jnp.float32) * scale
    return jnp.where(causal_mask, product, masked_value)

def log_total(logits, causal_mask):
    row_max = lax.optimization_barrier(jnp.max(logits, axis=-1))
    weights = jnp.where(causal_mask, jnp.exp(logits - row_max[:, None]), 0.0)
    return row_max + jnp.log(lax.optimization_barrier(jnp.sum(weights, axis=-1)))

def reference(teacher_query, teacher_key, student_query, student_key, pair_table):
    teacher_q = teacher_query.reshape(SEQS, L, HT, DH)
    teacher_k = teacher_key.reshape(SEQS, L, KVT, DH)
    student_q = student_query.reshape(SEQS, L, HS, DH)
    student_k = student_key.reshape(SEQS, L, KVS, DH)
    group_teacher = HT // KVT
    group_student = HS // KVS
    positions = jnp.arange(L, dtype=jnp.int32)
    causal_mask = positions[None, :] <= positions[:, None]

    def one_item(flat_index):
        sequence = flat_index // HS
        student = flat_index % HS
        s_logits = masked_logits(student_q[sequence, :, student], student_k[sequence, :, student // group_student], causal_mask)
        s_lse = log_total(s_logits, causal_mask)
        total = jnp.zeros((L,), jnp.float32)
        for column in range(2):
            teacher = pair_table[student, column]
            t_logits = masked_logits(teacher_q[sequence, :, teacher], teacher_k[sequence, :, teacher // group_teacher], causal_mask)
            t_lse = log_total(t_logits, causal_mask)
            probs = jnp.where(causal_mask, jnp.exp(t_logits - t_lse[:, None]), 0.0)
            total = total + (lax.optimization_barrier(jnp.sum(probs * (t_logits - s_logits), axis=-1)) - t_lse + s_lse)
        return total
    kl = lax.map(one_item, jnp.arange(SEQS * HS, dtype=jnp.int32)).reshape(SEQS, HS, L)
    head_loss = lax.optimization_barrier(jnp.sum(kl, axis=(0, 2))) / (SEQS * L)
    return (kl, head_loss)
```

```python
import functools
import math

import jax
import jax.numpy as jnp
from jax import lax
from jax.experimental import pallas as pl
from jax.experimental.pallas import tpu as pltpu
from jax.sharding import PartitionSpec as P

HT = 28
KVT = 4
DH = 128
HS = 14
KVS = 2

MESH = pl.DeviceIdType.MESH
LOWEST = -1e30


def nn(a, b):
    return jnp.dot(a, b, preferred_element_type=jnp.float32)


def flip(x):
    n = x.shape[1]
    eye = (
        lax.broadcasted_iota(jnp.int32, (n, n), 0) == lax.broadcasted_iota(jnp.int32, (n, n), 1)
    ).astype(jnp.bfloat16)
    out = lax.dot_general(eye, x, (((1,), (1,)), ((), ())), preferred_element_type=jnp.float32)
    return out.astype(jnp.bfloat16)


def kernel(
    n_dp, n_head, n_kv, rows,
    table_hbm, tq_hbm, tk_hbm, sq_hbm, sk_hbm,
    kl_ref, loss_ref,
    tq, tk, sq, sk,
    tq_t, sq_t, key_t, mixed, t_max, s_max, s_sum,
    table, inverse, acc, acc_in, sums_out, sums,
    layer_sem, chain_sem, load_sem, x_send, x_recv, z_send, z_recv, sum_send, sum_recv,
):
    n_t, n_s = HT // n_head, HS // n_head
    g_t, g_s = KVT // n_head, KVS // n_head
    per_t, per_s = HT // KVT, HS // KVS
    dp, hd, kv = lax.axis_index("dp"), lax.axis_index("head"), lax.axis_index("kv")
    n_rank = n_dp * n_head * n_kv
    rank = (dp * n_head + hd) * n_kv + kv
    scale = 1.0 / math.sqrt(DH)
    rate = scale * math.log2(math.e)

    loads = [
        pltpu.make_async_copy(sk_hbm.at[0], sk.at[hd, kv], load_sem.at[0]),
        pltpu.make_async_copy(tk_hbm.at[0], tk.at[kv], load_sem.at[1]),
        pltpu.make_async_copy(sq_hbm.at[0], sq.at[hd], load_sem.at[2]),
        pltpu.make_async_copy(tq_hbm.at[0], tq, load_sem.at[3]),
        pltpu.make_async_copy(table_hbm, table, load_sem.at[4]),
    ]
    for load in loads:
        load.start()

    barrier = pltpu.get_barrier_semaphore()

    def coordinates(peer):
        return (peer // (n_head * n_kv), peer // n_kv % n_head, peer % n_kv)

    def greet(sem, **peer):
        pl.semaphore_signal(sem, inc=1, device_id=peer, device_id_type=MESH)

    first, last = kv == 0, kv == n_kv - 1
    for s in range(1, n_dp):
        greet(barrier, dp=(dp + s) % n_dp)
    for s in range(1, n_head):
        greet(barrier, head=(hd + s) % n_head)

    @pl.when(jnp.logical_not(first))
    def _():
        greet(barrier, kv=kv - 1)

    @pl.when(jnp.logical_not(last))
    def _():
        greet(barrier, kv=kv + 1)

    near = n_dp - 1 + n_head - 1 + (kv > 0).astype(jnp.int32) + (kv < n_kv - 1).astype(jnp.int32)

    for load in loads[:4]:
        load.wait()
    pl.semaphore_wait(barrier, near)

    def across(slot, step, src, dst):
        return pltpu.make_async_remote_copy(
            src_ref=src, dst_ref=dst, send_sem=x_send.at[slot, step - 1],
            recv_sem=x_recv.at[slot, step - 1],
            device_id={"head": (hd + step) % n_head}, device_id_type=MESH,
        )

    def upward(block, piece):
        ref = tk.at[block] if piece is n_head else sk.at[piece, block]
        return pltpu.make_async_remote_copy(
            src_ref=ref, dst_ref=ref, send_sem=z_send.at[block, piece],
            recv_sem=z_recv.at[block, piece],
            device_id={"kv": jnp.minimum(kv + 1, n_kv - 1)}, device_id_type=MESH,
        )

    def launch(piece):
        @pl.when(not_last)
        def _():
            upward(kv, piece).start()

    pieces = [n_head] + [(hd + s) % n_head for s in range(n_head)]
    not_last = kv < n_kv - 1

    keys_over = [across(0, s, sk.at[hd, kv], sk.at[hd, kv]) for s in range(1, n_head)]
    queries_over = [across(1, s, sq.at[hd], sq.at[hd]) for s in range(1, n_head)]
    for copy in keys_over:
        copy.start()

    launch(n_head)
    launch(hd)

    for copy in queries_over:
        copy.start()

    for s in range(1, n_head):
        greet(layer_sem, head=(hd + s) % n_head)
    loads[4].wait()
    entries = [table[k % 2, k // 2] for k in range(HT)]
    for t in range(n_t):
        found = jnp.int32(0)
        for k in range(HT):
            found = jnp.where(entries[k] == hd * n_t + t, k // 2, found)
        inverse[t] = found

    for h in range(n_t):
        tq_t[h] = flip(tq[:, h * DH:(h + 1) * DH])
    for h in range(n_s):
        sq_t[hd * n_s + h] = flip(sq[hd, :, h * DH:(h + 1) * DH])

    key_t[:, 2 * DH:] = jnp.ones((g_t * KVS, 16, rows), jnp.bfloat16)
    for copy in keys_over:
        copy.wait()

    for s in range(1, n_head):
        launch((hd + s) % n_head)

    pl.semaphore_wait(layer_sem, n_head - 1)

    @pl.when(jnp.logical_not(first))
    def _():
        pl.semaphore_wait(chain_sem.at[0], 1)

    @pl.when(jnp.logical_not(last))
    def _():
        greet(chain_sem.at[0], kv=kv + 1)

    visible = lax.broadcasted_iota(jnp.int32, (rows, rows), 0) <= lax.broadcasted_iota(
        jnp.int32, (rows, rows), 1
    )

    def fold(block, diagonal):
        for g in range(g_t):
            flipped = flip(tk[block, :, g * DH:(g + 1) * DH])
            for j in range(KVS):
                key_t[g * KVS + j, :DH] = flipped
        for j in range(KVS):
            flipped = flip(sk[j // g_s, block, :, j % g_s * DH:(j % g_s + 1) * DH])
            for g in range(g_t):
                key_t[g * KVS + j, DH:2 * DH] = flipped

        def weigh(logits, high, row):
            if diagonal:
                logits = jnp.where(visible, logits, LOWEST)
            top = jnp.max(logits, axis=0, keepdims=True)
            if diagonal:
                decay = None
            else:
                old = high[row]
                top = jnp.maximum(old, top)
                decay = jnp.exp2((old - top) * rate)
            weights = jnp.exp2((logits - top) * rate)
            high[row] = top
            return weights, decay

        for h in range(n_t):
            g = h // per_t
            logits = nn(tk[block, :, g * DH:(g + 1) * DH], tq_t[h])
            weights, decay = weigh(logits, t_max, h)
            part = nn(key_t[g * KVS + inverse[h] // per_s], weights.astype(jnp.bfloat16))
            mixed[h] = part if diagonal else mixed[h] * decay + part
        for h in range(n_s):
            g = h // per_s
            logits = nn(sk[hd, block, :, g * DH:(g + 1) * DH], sq_t[hd * n_s + h])
            weights, decay = weigh(logits, s_max, h)
            part = jnp.sum(weights, axis=0, keepdims=True)
            s_sum[h] = part if diagonal else s_sum[h] * decay + part

    fold(kv, True)

    @pl.when(jnp.logical_not(last))
    def _():
        pl.semaphore_wait(chain_sem.at[1], 1)

    @pl.when(jnp.logical_not(first))
    def _():
        greet(chain_sem.at[1], kv=kv - 1)

    def step(s, carry):
        block = kv - s
        for piece in pieces:
            upward(block, piece).wait_recv()

            @pl.when(not_last)
            def _():
                upward(block, piece).start()
        fold(block, False)
        return carry

    lax.fori_loop(1, kv + 1, step, 0)

    for copy in queries_over:
        copy.wait()
    for s in range(1, n_head):
        d = (hd + s) % n_head
        for h in range(n_s):
            sq_t[d * n_s + h] = flip(sq[d, :, h * DH:(h + 1) * DH])

    pad = acc.shape[0] // n_head
    place = lax.broadcasted_iota(jnp.int32, acc.shape, 0)
    total = jnp.zeros(acc.shape, jnp.float32)
    for h in range(n_t):
        partner = inverse[h]
        own = mixed[h, :DH] * tq_t[h].astype(jnp.float32)
        other = mixed[h, DH:2 * DH] * sq_t[partner].astype(jnp.float32)
        mass = mixed[h, 2 * DH:2 * DH + 1]
        value = jnp.sum(own - other, axis=0, keepdims=True) * scale / mass
        value = value - (t_max[h] * scale + jnp.log(mass))
        row = (partner // n_s) * pad + partner % n_s
        total = total + jnp.where(place == row, value, 0.0)
    acc[...] = total

    returns = [
        across(2, s, acc.at[pl.ds(((hd + s) % n_head) * pad, pad)], acc_in.at[s - 1])
        for s in range(1, n_head)
    ]
    for copy in returns:
        copy.start()
    lse = jnp.concatenate(
        [s_max[h] * scale + jnp.log(s_sum[h]) for h in range(n_s)]
        + [jnp.zeros((1, rows), jnp.float32)] * (pad - n_s),
        axis=0,
    )
    mine = jnp.where(place // pad == hd, 2.0 * jnp.concatenate([lse] * n_head, axis=0), 0.0)
    column = jnp.sum(total + mine, axis=1, keepdims=True)
    across_lanes = lax.broadcasted_iota(jnp.int32, (n_head * pad, 128), 1)
    down_rows = lax.broadcasted_iota(jnp.int32, (n_head * pad, 128), 0)
    for d in range(n_head):
        sums_out[d] = jnp.sum(
            jnp.where(down_rows == across_lanes + d * pad, column, 0.0), axis=0, keepdims=True
        )

    def share(peer, place):
        return pltpu.make_async_remote_copy(
            src_ref=sums_out.at[peer // n_kv % n_head], dst_ref=sums.at[rank],
            send_sem=sum_send.at[peer], recv_sem=sum_recv.at[place],
            device_id=coordinates(peer), device_id_type=MESH,
        )

    def send(peer, carry):
        @pl.when(peer != rank)
        def _():
            share(peer, rank).start()
        return carry

    def land(peer, carry):
        @pl.when(peer != rank)
        def _():
            share(peer, rank).wait_send()
            share(peer, peer).wait_recv()
        return carry

    lax.fori_loop(0, n_rank, send, 0)
    sums[rank] = sums_out[hd]
    kl = acc[pl.ds(hd * pad, pad)] + 2.0 * lse
    for s in range(1, n_head):
        returns[s - 1].wait()
        kl = kl + acc_in[s - 1]
    for h in range(n_s):
        kl_ref[h] = kl[h:h + 1]

    @pl.when(not_last)
    def _():
        def drain(block, carry):
            for piece in pieces:
                upward(block, piece).wait_send()
            return carry
        lax.fori_loop(0, kv + 1, drain, 0)

    lax.fori_loop(0, n_rank, land, 0)
    line = jnp.sum(sums[...], axis=0)
    loss_ref[...] = line[:, :n_s] / (n_dp * rows * n_kv)


def finish(kl_in, loss_in, kl_ref, loss_ref):
    kl_ref[...] = kl_in[...]
    loss_ref[...] = loss_in[...]


def per_device(teacher_query, teacher_key, student_query, student_key, pair_table):
    n_dp, n_head, n_kv = lax.axis_size("dp"), lax.axis_size("head"), lax.axis_size("kv")
    seq_dev, rows, wide_t = teacher_query.shape
    assert seq_dev == 1
    n_t, n_s = HT // n_head, HS // n_head
    g_t, g_s = KVT // n_head, KVS // n_head
    n_rank = n_dp * n_head * n_kv
    pad = -(-n_s // 8) * 8
    f32, bf16 = jnp.float32, jnp.bfloat16
    dma = pltpu.SemaphoreType.DMA
    kl, loss = pl.pallas_call(
        functools.partial(kernel, n_dp, n_head, n_kv, rows),
        out_shape=(
            jax.ShapeDtypeStruct((n_s, 1, rows), f32),
            jax.ShapeDtypeStruct((1, n_s), f32),
        ),
        in_specs=[pl.BlockSpec(memory_space=pl.ANY)] * 5,
        out_specs=(
            pl.BlockSpec(memory_space=pltpu.VMEM),
            pl.BlockSpec(memory_space=pltpu.VMEM),
        ),
        scratch_shapes=[
            pltpu.VMEM((rows, wide_t), bf16),
            pltpu.VMEM((n_kv, rows, g_t * DH), bf16),
            pltpu.VMEM((n_head, rows, n_s * DH), bf16),
            pltpu.VMEM((n_head, n_kv, rows, g_s * DH), bf16),
            pltpu.VMEM((n_t, DH, rows), bf16),
            pltpu.VMEM((HS, DH, rows), bf16),
            pltpu.VMEM((g_t * KVS, 2 * DH + 16, rows), bf16),
            pltpu.VMEM((n_t, 2 * DH + 16, rows), f32),
            pltpu.VMEM((n_t, 1, rows), f32),
            pltpu.VMEM((n_s, 1, rows), f32),
            pltpu.VMEM((n_s, 1, rows), f32),
            pltpu.SMEM(pair_table.shape[::-1], jnp.int32),
            pltpu.SMEM((n_t,), jnp.int32),
            pltpu.VMEM((n_head * pad, rows), f32),
            pltpu.VMEM((max(n_head - 1, 1), pad, rows), f32),
            pltpu.VMEM((n_head, 1, 128), f32),
            pltpu.VMEM((n_rank, 1, 128), f32),
            pltpu.SemaphoreType.REGULAR,
            pltpu.SemaphoreType.REGULAR((2,)),
            dma((5,)),
            dma((3, max(n_head - 1, 1))),
            dma((3, max(n_head - 1, 1))),
            dma((n_kv, n_head + 1)),
            dma((n_kv, n_head + 1)),
            dma((n_rank,)),
            dma((n_rank,)),
        ],
        compiler_params=pltpu.CompilerParams(collective_id=0, has_side_effects=True),
    )(pair_table.T, teacher_query, teacher_key, student_query, student_key)
    kl, loss = pl.pallas_call(
        finish,
        out_shape=(
            jax.ShapeDtypeStruct((n_s, 1, rows), f32),
            jax.ShapeDtypeStruct((1, n_s), f32),
        ),
        in_specs=[pl.BlockSpec(memory_space=pltpu.VMEM)] * 2,
        out_specs=(
            pl.BlockSpec(memory_space=pltpu.VMEM),
            pl.BlockSpec(memory_space=pltpu.VMEM),
        ),
    )(kl, loss)
    return kl.reshape(1, n_s, rows), loss.reshape(n_s)


def solution(mesh):
    split = P("dp", "kv", "head")
    return jax.shard_map(
        per_device,
        mesh=mesh,
        in_specs=(split, split, split, split, P()),
        out_specs=(P("dp", "head", "kv"), P("head")),
        check_vma=False,
    )
```

```python
import functools
import math

import jax
import jax.numpy as jnp
from jax import lax
from jax.experimental import pallas as pl
from jax.experimental.pallas import tpu as pltpu
from jax.sharding import PartitionSpec as P

HT = 28
KVT = 4
DH = 128
HS = 14
KVS = 2

MESH = pl.DeviceIdType.MESH
LOWEST = -1e30


def nn(a, b):
    return jnp.dot(a, b, preferred_element_type=jnp.float32)


def flip(x):
    n = x.shape[1]
    eye = (
        lax.broadcasted_iota(jnp.int32, (n, n), 0) == lax.broadcasted_iota(jnp.int32, (n, n), 1)
    ).astype(jnp.bfloat16)
    out = lax.dot_general(eye, x, (((1,), (1,)), ((), ())), preferred_element_type=jnp.float32)
    return out.astype(jnp.bfloat16)


def kernel(
    n_dp, n_head, n_kv, rows, shared,
    table_hbm, tq_hbm, tk_hbm, sq_hbm, sk_hbm,
    kl_ref, loss_ref,
    tq, tk, sq, sk,
    tq_t, sq_t, tk_t, sk_t, weights, mixed_t, mixed_s, t_max, t_decay, s_max, s_sum,
    table, inverse, acc, acc_in, sums_out, sums,
    layer_sem, chain_sem, load_sem, key_send, key_recv, query_send, query_recv,
    back_send, back_recv, z_send, z_recv, sum_send, sum_recv,
):
    n_t, n_s = HT // n_head, HS // n_head
    g_t, g_s = KVT // n_head, KVS // n_head
    per_t, per_s = HT // KVT, HS // KVS
    dp, hd, kv = lax.axis_index("dp"), lax.axis_index("head"), lax.axis_index("kv")
    n_rank = n_dp * n_head * n_kv
    rank = (dp * n_head + hd) * n_kv + kv
    scale = 1.0 / math.sqrt(DH)
    rate = scale * math.log2(math.e)
    bf16 = jnp.bfloat16

    loads = [
        pltpu.make_async_copy(sk_hbm.at[0], sk.at[hd, kv], load_sem.at[0]),
        pltpu.make_async_copy(tk_hbm.at[0], tk.at[kv], load_sem.at[1]),
        pltpu.make_async_copy(sq_hbm.at[0], sq.at[hd], load_sem.at[2]),
        pltpu.make_async_copy(table_hbm, table, load_sem.at[3]),
        pltpu.make_async_copy(tq_hbm.at[0], tq, load_sem.at[4]),
    ]
    for load in loads:
        load.start()

    first, last = kv == 0, kv == n_kv - 1
    not_first, not_last = kv > 0, kv < n_kv - 1
    barrier = pltpu.get_barrier_semaphore()

    def greet(sem, **peer):
        pl.semaphore_signal(sem, inc=1, device_id=peer, device_id_type=MESH)

    @pl.when(not_first)
    def _():
        greet(barrier, kv=kv - 1)

    @pl.when(not_last)
    def _():
        greet(barrier, kv=kv + 1)

    for s in range(1, n_head):
        greet(barrier, head=(hd + s) % n_head)
    for s in range(1, n_dp):
        greet(barrier, dp=(dp + s) % n_dp)

    def column(step):
        return (hd + step) % n_head

    def across(step, src, dst, send, recv):
        return pltpu.make_async_remote_copy(
            src_ref=src, dst_ref=dst, send_sem=send, recv_sem=recv,
            device_id={"head": column(step)}, device_id_type=MESH,
        )

    def keys_over(block):
        return [
            across(
                s, sk.at[hd, block], sk.at[hd, block],
                key_send.at[block, s - 1], key_recv.at[block, s - 1],
            )
            for s in range(1, n_head)
        ]

    cuts = [0, n_s * 2 // 7, n_s * 4 // 7, n_s]
    n_group = len(cuts) - 1

    def queries_over(group):
        part = sq.at[hd, :, cuts[group] * DH:cuts[group + 1] * DH]
        return [
            across(s, part, part, query_send.at[group, s - 1], query_recv.at[group, s - 1])
            for s in range(1, n_head)
        ]

    def start(copies):
        for copy in copies:
            copy.start()

    def upward(block, piece):
        ref = tk.at[block] if piece == n_head else sk.at[column(piece), block]
        return pltpu.make_async_remote_copy(
            src_ref=ref, dst_ref=ref, send_sem=z_send.at[block, piece],
            recv_sem=z_recv.at[block, piece],
            device_id={"kv": jnp.minimum(kv + 1, n_kv - 1)}, device_id_type=MESH,
        )

    def launch(block, piece):
        @pl.when(not_last)
        def _():
            upward(block, piece).start()

    def land(block, piece):
        upward(block, piece).wait_recv()
        launch(block, piece)

    def receive_own(block):
        @pl.when(block >= shared)
        def _():
            land(block, 0)
            start(keys_over(block))

    def receive_rest(block):
        land(block, n_head)

        @pl.when(block < shared)
        def _():
            land(block, 0)
            for s in range(1, n_head):
                land(block, s)

    loads[0].wait()
    loads[1].wait()
    pl.semaphore_wait(
        barrier, n_dp - 1 + n_head - 1 + not_first.astype(jnp.int32) + not_last.astype(jnp.int32)
    )
    start(keys_over(kv))

    @pl.when(kv < shared)
    def _():
        launch(kv, n_head)
        launch(kv, 0)

    @pl.when(kv >= shared)
    def _():
        launch(kv, 0)
        launch(kv, n_head)

    loads[2].wait()
    start(queries_over(0))
    for s in range(1, n_head):
        greet(layer_sem, head=column(s))

    loads[3].wait()
    entries = [table[k % 2, k // 2] for k in range(HT)]
    for t in range(n_t):
        found = jnp.int32(0)
        for k in range(HT):
            found = jnp.where(entries[k] == hd * n_t + t, k // 2, found)
        inverse[t] = found

    loads[4].wait()
    for h in range(n_t):
        tq_t[h] = flip(tq[:, h * DH:(h + 1) * DH])
    for h in range(n_s):
        sq_t[hd * n_s + h] = flip(sq[hd, :, h * DH:(h + 1) * DH])
    tk_t[:, DH:] = jnp.ones((g_t, 16, rows), bf16)

    for copy in keys_over(kv):
        copy.wait_recv()

    @pl.when(kv < shared)
    def _():
        for s in range(1, n_head):
            launch(kv, s)

    @pl.when(not_last & not_first)
    def _():
        receive_own(kv - 1)
        receive_rest(kv - 1)

    pl.semaphore_wait(layer_sem, n_head - 1)

    @pl.when(not_first)
    def _():
        pl.semaphore_wait(chain_sem.at[0], 1)

    @pl.when(not_last)
    def _():
        greet(chain_sem.at[0], kv=kv + 1)

    visible = lax.broadcasted_iota(jnp.int32, (rows, rows), 0) <= lax.broadcasted_iota(
        jnp.int32, (rows, rows), 1
    )

    def fold(block, diagonal, between):
        def weigh(logits, high, row):
            if diagonal:
                logits = jnp.where(visible, logits, LOWEST)
            top = jnp.max(logits, axis=0, keepdims=True)
            if diagonal:
                decay = None
            else:
                old = high[row]
                top = jnp.maximum(old, top)
                decay = jnp.exp2((old - top) * rate)
            high[row] = top
            return jnp.exp2((logits - top) * rate), decay

        if not diagonal:
            @pl.when(last)
            def _():
                upward(block, n_head).wait_recv()

        for g in range(g_t):
            tk_t[g, :DH] = flip(tk[block, :, g * DH:(g + 1) * DH])
        for h in range(n_t):
            g = h // per_t
            logits = nn(tk[block, :, g * DH:(g + 1) * DH], tq_t[h])
            weight, decay = weigh(logits, t_max, h)
            weight = weight.astype(bf16)
            weights[h] = weight
            part = nn(tk_t[g], weight)
            if diagonal:
                mixed_t[h] = part
            else:
                t_decay[h] = decay
                mixed_t[h] = mixed_t[h] * decay + part

        between()
        if not diagonal:
            @pl.when(last & (block < shared))
            def _():
                upward(block, 0).wait_recv()

        for h in range(n_s):
            g = h // per_s
            logits = nn(sk[hd, block, :, g * DH:(g + 1) * DH], sq_t[hd * n_s + h])
            weight, decay = weigh(logits, s_max, h)
            part = jnp.sum(weight, axis=0, keepdims=True)
            s_sum[h] = part if diagonal else s_sum[h] * decay + part

        if not diagonal:
            @pl.when(last & (block < shared))
            def _():
                for s in range(1, n_head):
                    upward(block, s).wait_recv()

            @pl.when(block >= shared)
            def _():
                for copy in keys_over(block):
                    copy.wait_recv()

        for j in range(KVS):
            sk_t[j] = flip(sk[j // g_s, block, :, j % g_s * DH:(j % g_s + 1) * DH])
        for h in range(n_t):
            part = nn(sk_t[inverse[h] // per_s], weights[h])
            mixed_s[h] = part if diagonal else mixed_s[h] * t_decay[h] + part

    def after_own():
        @pl.when(last & not_first)
        def _():
            receive_own(kv - 1)

        start(queries_over(1))

        @pl.when(first)
        def _():
            start(queries_over(2))

    fold(kv, True, after_own)

    @pl.when(not_last)
    def _():
        pl.semaphore_wait(chain_sem.at[1], 1)

    @pl.when(not_first)
    def _():
        greet(chain_sem.at[1], kv=kv - 1)

    def step(s, carry):
        block = kv - s

        @pl.when(not_last & (s < kv))
        def _():
            receive_own(block - 1)
            receive_rest(block - 1)

        def between():
            @pl.when(last & (s < kv))
            def _():
                receive_own(block - 1)

            @pl.when(s == 1)
            def _():
                start(queries_over(2))

        fold(block, False, between)
        return carry

    lax.fori_loop(1, kv + 1, step, 0)

    for group in range(n_group):
        for copy in queries_over(group):
            copy.wait_recv()
        for s in range(1, n_head):
            for h in range(cuts[group], cuts[group + 1]):
                sq_t[column(s) * n_s + h] = flip(sq[column(s), :, h * DH:(h + 1) * DH])

    pad = acc.shape[0] // n_head
    place = lax.broadcasted_iota(jnp.int32, acc.shape, 0)
    total = jnp.zeros(acc.shape, jnp.float32)
    for h in range(n_t):
        partner = inverse[h]
        own = mixed_t[h, :DH] * tq_t[h].astype(jnp.float32)
        other = mixed_s[h] * sq_t[partner].astype(jnp.float32)
        mass = mixed_t[h, DH:DH + 1]
        value = jnp.sum(own - other, axis=0, keepdims=True) * scale / mass
        value = value - (t_max[h] * scale + jnp.log(mass))
        row = (partner // n_s) * pad + partner % n_s
        total = total + jnp.where(place == row, value, 0.0)
    acc[...] = total

    returns = [
        across(
            s, acc.at[pl.ds(column(s) * pad, pad)], acc_in.at[s - 1],
            back_send.at[s - 1], back_recv.at[s - 1],
        )
        for s in range(1, n_head)
    ]
    start(returns)
    lse = jnp.concatenate(
        [s_max[h] * scale + jnp.log(s_sum[h]) for h in range(n_s)]
        + [jnp.zeros((1, rows), jnp.float32)] * (pad - n_s),
        axis=0,
    )
    mine = jnp.where(place // pad == hd, 2.0 * jnp.concatenate([lse] * n_head, axis=0), 0.0)
    side = jnp.sum(total + mine, axis=1, keepdims=True)
    across_lanes = lax.broadcasted_iota(jnp.int32, (n_head * pad, 128), 1)
    down_rows = lax.broadcasted_iota(jnp.int32, (n_head * pad, 128), 0)
    for d in range(n_head):
        sums_out[d] = jnp.sum(
            jnp.where(down_rows == across_lanes + d * pad, side, 0.0), axis=0, keepdims=True
        )

    def share(d, h, k):
        return pltpu.make_async_remote_copy(
            src_ref=sums_out.at[h], dst_ref=sums.at[rank],
            send_sem=sum_send, recv_sem=sum_recv,
            device_id=(d, h, k), device_id_type=MESH,
        )

    def each_peer(act):
        def outer(k, carry):
            def middle(d, carry):
                for h in range(n_head):
                    @pl.when((d * n_head + h) * n_kv + k != rank)
                    def _():
                        act(d, h, k)
                return carry
            return lax.fori_loop(0, n_dp, middle, carry)
        lax.fori_loop(0, n_kv, outer, 0)

    each_peer(lambda d, h, k: share(d, h, k).start())
    sums[rank] = sums_out[hd]
    kl = acc[pl.ds(hd * pad, pad)] + 2.0 * lse
    for s in range(1, n_head):
        returns[s - 1].wait()
        kl = kl + acc_in[s - 1]
    for h in range(n_s):
        kl_ref[h] = kl[h:h + 1]

    for group in range(n_group):
        for copy in queries_over(group):
            copy.wait_send()

    def drain(block, carry):
        @pl.when((block >= shared) | (block == kv))
        def _():
            for copy in keys_over(block):
                copy.wait_send()

        @pl.when(not_last)
        def _():
            upward(block, 0).wait_send()
            upward(block, n_head).wait_send()

            @pl.when(block < shared)
            def _():
                for s in range(1, n_head):
                    upward(block, s).wait_send()
        return carry

    lax.fori_loop(0, kv + 1, drain, 0)

    others = sums.at[pl.ds(0, n_rank - 1)]
    pltpu.make_async_remote_copy(
        src_ref=others, dst_ref=others, send_sem=sum_send, recv_sem=sum_recv,
        device_id={"head": column(1)}, device_id_type=MESH,
    ).wait()
    line = jnp.sum(sums[...], axis=0)
    loss_ref[...] = line[:, :n_s] / (n_dp * rows * n_kv)


def finish(kl_in, loss_in, kl_ref, loss_ref):
    kl_ref[...] = kl_in[...]
    loss_ref[...] = loss_in[...]


def per_device(teacher_query, teacher_key, student_query, student_key, pair_table):
    n_dp, n_head, n_kv = lax.axis_size("dp"), lax.axis_size("head"), lax.axis_size("kv")
    seq_dev, rows, wide_t = teacher_query.shape
    assert seq_dev == 1
    n_t, n_s = HT // n_head, HS // n_head
    g_t, g_s = KVT // n_head, KVS // n_head
    n_rank = n_dp * n_head * n_kv
    pad = -(-n_s // 8) * 8
    key_t, key_s, query_s = g_t * DH, g_s * DH, n_s * DH
    spare = query_s + n_kv * key_s - (n_kv - 1) * (key_t + key_s)
    shared = min(max(round(spare / (2 * key_s * max(n_head - 1, 1))), 0), n_kv - 1)
    f32, bf16 = jnp.float32, jnp.bfloat16
    dma = pltpu.SemaphoreType.DMA
    kl, loss = pl.pallas_call(
        functools.partial(kernel, n_dp, n_head, n_kv, rows, shared),
        out_shape=(
            jax.ShapeDtypeStruct((n_s, 1, rows), f32),
            jax.ShapeDtypeStruct((1, n_s), f32),
        ),
        in_specs=[pl.BlockSpec(memory_space=pl.ANY)] * 5,
        out_specs=(
            pl.BlockSpec(memory_space=pltpu.VMEM),
            pl.BlockSpec(memory_space=pltpu.VMEM),
        ),
        scratch_shapes=[
            pltpu.VMEM((rows, wide_t), bf16),
            pltpu.VMEM((n_kv, rows, g_t * DH), bf16),
            pltpu.VMEM((n_head, rows, n_s * DH), bf16),
            pltpu.VMEM((n_head, n_kv, rows, g_s * DH), bf16),
            pltpu.VMEM((n_t, DH, rows), bf16),
            pltpu.VMEM((HS, DH, rows), bf16),
            pltpu.VMEM((g_t, DH + 16, rows), bf16),
            pltpu.VMEM((KVS, DH, rows), bf16),
            pltpu.VMEM((n_t, rows, rows), bf16),
            pltpu.VMEM((n_t, DH + 16, rows), f32),
            pltpu.VMEM((n_t, DH, rows), f32),
            pltpu.VMEM((n_t, 1, rows), f32),
            pltpu.VMEM((n_t, 1, rows), f32),
            pltpu.VMEM((n_s, 1, rows), f32),
            pltpu.VMEM((n_s, 1, rows), f32),
            pltpu.SMEM(pair_table.shape[::-1], jnp.int32),
            pltpu.SMEM((n_t,), jnp.int32),
            pltpu.VMEM((n_head * pad, rows), f32),
            pltpu.VMEM((max(n_head - 1, 1), pad, rows), f32),
            pltpu.VMEM((n_head, 1, 128), f32),
            pltpu.VMEM((n_rank, 1, 128), f32),
            pltpu.SemaphoreType.REGULAR,
            pltpu.SemaphoreType.REGULAR((2,)),
            dma((5,)),
            dma((n_kv, max(n_head - 1, 1))),
            dma((n_kv, max(n_head - 1, 1))),
            dma((3, max(n_head - 1, 1))),
            dma((3, max(n_head - 1, 1))),
            dma((max(n_head - 1, 1),)),
            dma((max(n_head - 1, 1),)),
            dma((n_kv, n_head + 1)),
            dma((n_kv, n_head + 1)),
            dma(()),
            dma(()),
        ],
        compiler_params=pltpu.CompilerParams(collective_id=0, has_side_effects=True),
    )(pair_table.T, teacher_query, teacher_key, student_query, student_key)
    kl, loss = pl.pallas_call(
        finish,
        out_shape=(
            jax.ShapeDtypeStruct((n_s, 1, rows), f32),
            jax.ShapeDtypeStruct((1, n_s), f32),
        ),
        in_specs=[pl.BlockSpec(memory_space=pltpu.VMEM)] * 2,
        out_specs=(
            pl.BlockSpec(memory_space=pltpu.VMEM),
            pl.BlockSpec(memory_space=pltpu.VMEM),
        ),
    )(kl, loss)
    return kl.reshape(1, n_s, rows), loss.reshape(n_s)


def solution(mesh):
    split = P("dp", "kv", "head")
    return jax.shard_map(
        per_device,
        mesh=mesh,
        in_specs=(split, split, split, split, P()),
        out_specs=(P("dp", "head", "kv"), P("head")),
        check_vma=False,
    )
```

```python
import functools
import math

import jax
import jax.numpy as jnp
from jax import lax
from jax.experimental import pallas as pl
from jax.experimental.pallas import tpu as pltpu
from jax.sharding import PartitionSpec as P

HT = 28
KVT = 4
DH = 128
HS = 14
KVS = 2

MESH = pl.DeviceIdType.MESH
LOWEST = -1e30


def nn(a, b):
    return jnp.dot(a, b, preferred_element_type=jnp.float32)


def flip(x):
    n = x.shape[1]
    eye = (
        lax.broadcasted_iota(jnp.int32, (n, n), 0) == lax.broadcasted_iota(jnp.int32, (n, n), 1)
    ).astype(jnp.bfloat16)
    out = lax.dot_general(eye, x, (((1,), (1,)), ((), ())), preferred_element_type=jnp.float32)
    return out.astype(jnp.bfloat16)


def kernel(
    n_dp, n_head, n_kv, rows, shared,
    table_hbm, tq_hbm, tk_hbm, sq_hbm, sk_hbm,
    kl_ref, loss_ref,
    tq, tk, sq, sk,
    tq_t, sq_t, key_t, weights, mixed, t_max, t_decay, s_max, s_sum,
    table, inverse, acc, acc_in, sums_out, sums,
    layer_sem, chain_sem, load_sem, key_send, key_recv, query_send, query_recv,
    back_send, back_recv, z_send, z_recv, sum_send, sum_recv,
):
    n_t, n_s = HT // n_head, HS // n_head
    g_t, g_s = KVT // n_head, KVS // n_head
    per_t, per_s = HT // KVT, HS // KVS
    dp, hd, kv = lax.axis_index("dp"), lax.axis_index("head"), lax.axis_index("kv")
    n_rank = n_dp * n_head * n_kv
    rank = (dp * n_head + hd) * n_kv + kv
    scale = 1.0 / math.sqrt(DH)
    rate = scale * math.log2(math.e)
    bf16 = jnp.bfloat16

    loads = [
        pltpu.make_async_copy(sk_hbm.at[0], sk.at[hd, kv], load_sem.at[0]),
        pltpu.make_async_copy(tk_hbm.at[0], tk.at[kv], load_sem.at[1]),
        pltpu.make_async_copy(sq_hbm.at[0], sq.at[hd], load_sem.at[2]),
        pltpu.make_async_copy(table_hbm, table, load_sem.at[3]),
        pltpu.make_async_copy(tq_hbm.at[0], tq, load_sem.at[4]),
    ]
    for load in loads:
        load.start()

    first, last = kv == 0, kv == n_kv - 1
    not_first, not_last = kv > 0, kv < n_kv - 1
    barrier = pltpu.get_barrier_semaphore()

    def greet(sem, **peer):
        pl.semaphore_signal(sem, inc=1, device_id=peer, device_id_type=MESH)

    @pl.when(not_first)
    def _():
        greet(barrier, kv=kv - 1)

    @pl.when(not_last)
    def _():
        greet(barrier, kv=kv + 1)

    for s in range(1, n_head):
        greet(barrier, head=(hd + s) % n_head)
    for s in range(1, n_dp):
        greet(barrier, dp=(dp + s) % n_dp)

    def column(step):
        return (hd + step) % n_head

    def across(step, src, dst, send, recv):
        return pltpu.make_async_remote_copy(
            src_ref=src, dst_ref=dst, send_sem=send, recv_sem=recv,
            device_id={"head": column(step)}, device_id_type=MESH,
        )

    def keys_over(block):
        return [
            across(
                s, sk.at[hd, block], sk.at[hd, block],
                key_send.at[block, s - 1], key_recv.at[block, s - 1],
            )
            for s in range(1, n_head)
        ]

    cuts = [0, n_s * 2 // 7, n_s * 4 // 7, n_s]
    n_group = len(cuts) - 1

    def queries_over(group):
        part = sq.at[hd, :, cuts[group] * DH:cuts[group + 1] * DH]
        return [
            across(s, part, part, query_send.at[group, s - 1], query_recv.at[group, s - 1])
            for s in range(1, n_head)
        ]

    def start(copies):
        for copy in copies:
            copy.start()

    def upward(block, piece):
        ref = tk.at[block] if piece == n_head else sk.at[column(piece), block]
        return pltpu.make_async_remote_copy(
            src_ref=ref, dst_ref=ref, send_sem=z_send.at[block, piece],
            recv_sem=z_recv.at[block, piece],
            device_id={"kv": jnp.minimum(kv + 1, n_kv - 1)}, device_id_type=MESH,
        )

    def launch(block, piece):
        @pl.when(not_last)
        def _():
            upward(block, piece).start()

    def land(block, piece):
        upward(block, piece).wait_recv()
        launch(block, piece)

    def receive_own(block):
        @pl.when(block >= shared)
        def _():
            land(block, 0)
            start(keys_over(block))

    def receive_rest(block):
        land(block, n_head)

        @pl.when(block < shared)
        def _():
            land(block, 0)
            for s in range(1, n_head):
                land(block, s)

    loads[0].wait()
    loads[1].wait()
    pl.semaphore_wait(
        barrier, n_dp - 1 + n_head - 1 + not_first.astype(jnp.int32) + not_last.astype(jnp.int32)
    )
    start(keys_over(kv))

    @pl.when(kv < shared)
    def _():
        launch(kv, n_head)
        launch(kv, 0)

    @pl.when(kv >= shared)
    def _():
        launch(kv, 0)
        launch(kv, n_head)

    loads[2].wait()
    start(queries_over(0))
    for s in range(1, n_head):
        greet(layer_sem, head=column(s))

    loads[3].wait()
    entries = [table[k % 2, k // 2] for k in range(HT)]
    for t in range(n_t):
        found = jnp.int32(0)
        for k in range(HT):
            found = jnp.where(entries[k] == hd * n_t + t, k // 2, found)
        inverse[t] = found

    loads[4].wait()
    for h in range(n_t):
        tq_t[h] = flip(tq[:, h * DH:(h + 1) * DH])
    for h in range(n_s):
        sq_t[hd * n_s + h] = flip(sq[hd, :, h * DH:(h + 1) * DH])
    key_t[:, 2 * DH:] = jnp.ones((g_t * KVS, 16, rows), bf16)
    mixed[...] = jnp.zeros(mixed.shape, jnp.float32)

    for copy in keys_over(kv):
        copy.wait_recv()

    @pl.when(kv < shared)
    def _():
        for s in range(1, n_head):
            launch(kv, s)

    @pl.when(not_last & not_first)
    def _():
        receive_own(kv - 1)
        receive_rest(kv - 1)

    pl.semaphore_wait(layer_sem, n_head - 1)

    @pl.when(not_first)
    def _():
        pl.semaphore_wait(chain_sem.at[0], 1)

    @pl.when(not_last)
    def _():
        greet(chain_sem.at[0], kv=kv + 1)

    visible = lax.broadcasted_iota(jnp.int32, (rows, rows), 0) <= lax.broadcasted_iota(
        jnp.int32, (rows, rows), 1
    )

    def weigh(logits, high, row, diagonal):
        if diagonal:
            logits = jnp.where(visible, logits, LOWEST)
        top = jnp.max(logits, axis=0, keepdims=True)
        if diagonal:
            decay = jnp.zeros_like(top)
        else:
            old = high[row]
            top = jnp.maximum(old, top)
            decay = jnp.exp2((old - top) * rate)
        high[row] = top
        return jnp.exp2((logits - top) * rate), decay

    def turn_student(c, block):
        for j in range(g_s):
            flipped = flip(sk[c, block, :, j * DH:(j + 1) * DH])
            for g in range(g_t):
                key_t[g * KVS + c * g_s + j, DH:2 * DH] = flipped

    def weigh_block(block, diagonal):
        if not diagonal:
            @pl.when(last)
            def _():
                upward(block, n_head).wait_recv()

        for h in range(n_t):
            g = h // per_t
            logits = nn(tk[block, :, g * DH:(g + 1) * DH], tq_t[h])
            weight, t_decay[h] = weigh(logits, t_max, h, diagonal)
            weights[h] = weight.astype(bf16)
        for g in range(g_t):
            flipped = flip(tk[block, :, g * DH:(g + 1) * DH])
            for j in range(KVS):
                key_t[g * KVS + j, :DH] = flipped

        if not diagonal:
            @pl.when(last & (block < shared))
            def _():
                upward(block, 0).wait_recv()

        for h in range(n_s):
            g = h // per_s
            logits = nn(sk[hd, block, :, g * DH:(g + 1) * DH], sq_t[hd * n_s + h])
            weight, decay = weigh(logits, s_max, h, diagonal)
            part = jnp.sum(weight, axis=0, keepdims=True)
            s_sum[h] = part if diagonal else s_sum[h] * decay + part
        turn_student(hd, block)

    def await_others(block):
        @pl.when((block < shared) & last & not_first & (block != kv))
        def _():
            for s in range(1, n_head):
                upward(block, s).wait_recv()

        @pl.when((block >= shared) & (block != kv))
        def _():
            for copy in keys_over(block):
                copy.wait_recv()

        for s in range(1, n_head):
            turn_student(column(s), block)

    def mix(h):
        part = nn(key_t[h // per_t * KVS + inverse[h] // per_s], weights[h])
        return mixed[h] * t_decay[h] + part

    def after_own():
        @pl.when(last & not_first)
        def _():
            receive_own(kv - 1)

        start(queries_over(1))

        @pl.when(first)
        def _():
            start(queries_over(2))

    weigh_block(kv, True)
    after_own()

    @pl.when(not_last)
    def _():
        pl.semaphore_wait(chain_sem.at[1], 1)

    @pl.when(not_first)
    def _():
        greet(chain_sem.at[1], kv=kv - 1)

    def step(s, carry):
        block = kv - s

        @pl.when(not_last & (s < kv))
        def _():
            receive_own(block - 1)
            receive_rest(block - 1)

        await_others(block + 1)
        for h in range(n_t):
            mixed[h] = mix(h)
        weigh_block(block, False)

        @pl.when(last & (s < kv))
        def _():
            receive_own(block - 1)

        @pl.when(s == 1)
        def _():
            start(queries_over(2))

        return carry

    lax.fori_loop(1, kv + 1, step, 0)

    for group in range(n_group):
        for copy in queries_over(group):
            copy.wait_recv()
        for s in range(1, n_head):
            for h in range(cuts[group], cuts[group + 1]):
                sq_t[column(s) * n_s + h] = flip(sq[column(s), :, h * DH:(h + 1) * DH])

    await_others(0)
    pad = acc.shape[0] // n_head
    place = lax.broadcasted_iota(jnp.int32, acc.shape, 0)
    total = jnp.zeros(acc.shape, jnp.float32)
    for h in range(n_t):
        partner = inverse[h]
        blend = mix(h)
        own = blend[:DH] * tq_t[h].astype(jnp.float32)
        other = blend[DH:2 * DH] * sq_t[partner].astype(jnp.float32)
        mass = blend[2 * DH:2 * DH + 1]
        value = jnp.sum(own - other, axis=0, keepdims=True) * scale / mass
        value = value - (t_max[h] * scale + jnp.log(mass))
        row = (partner // n_s) * pad + partner % n_s
        total = total + jnp.where(place == row, value, 0.0)
    acc[...] = total

    returns = [
        across(
            s, acc.at[pl.ds(column(s) * pad, pad)], acc_in.at[s - 1],
            back_send.at[s - 1], back_recv.at[s - 1],
        )
        for s in range(1, n_head)
    ]
    start(returns)
    lse = jnp.concatenate(
        [s_max[h] * scale + jnp.log(s_sum[h]) for h in range(n_s)]
        + [jnp.zeros((1, rows), jnp.float32)] * (pad - n_s),
        axis=0,
    )
    mine = jnp.where(place // pad == hd, 2.0 * jnp.concatenate([lse] * n_head, axis=0), 0.0)
    side = jnp.sum(total + mine, axis=1, keepdims=True)
    across_lanes = lax.broadcasted_iota(jnp.int32, (n_head * pad, 128), 1)
    down_rows = lax.broadcasted_iota(jnp.int32, (n_head * pad, 128), 0)
    for d in range(n_head):
        sums_out[d] = jnp.sum(
            jnp.where(down_rows == across_lanes + d * pad, side, 0.0), axis=0, keepdims=True
        )

    def share(d, h, k):
        return pltpu.make_async_remote_copy(
            src_ref=sums_out.at[h], dst_ref=sums.at[rank],
            send_sem=sum_send, recv_sem=sum_recv,
            device_id=(d, h, k), device_id_type=MESH,
        )

    def each_peer(act):
        def outer(k, carry):
            def middle(d, carry):
                for h in range(n_head):
                    @pl.when((d * n_head + h) * n_kv + k != rank)
                    def _():
                        act(d, h, k)
                return carry
            return lax.fori_loop(0, n_dp, middle, carry)
        lax.fori_loop(0, n_kv, outer, 0)

    each_peer(lambda d, h, k: share(d, h, k).start())
    sums[rank] = sums_out[hd]
    kl = acc[pl.ds(hd * pad, pad)] + 2.0 * lse
    for s in range(1, n_head):
        returns[s - 1].wait()
        kl = kl + acc_in[s - 1]
    for h in range(n_s):
        kl_ref[h] = kl[h:h + 1]

    for group in range(n_group):
        for copy in queries_over(group):
            copy.wait_send()

    def drain(block, carry):
        @pl.when((block >= shared) | (block == kv))
        def _():
            for copy in keys_over(block):
                copy.wait_send()

        @pl.when(not_last)
        def _():
            upward(block, 0).wait_send()
            upward(block, n_head).wait_send()

            @pl.when(block < shared)
            def _():
                for s in range(1, n_head):
                    upward(block, s).wait_send()
        return carry

    lax.fori_loop(0, kv + 1, drain, 0)

    others = sums.at[pl.ds(0, n_rank - 1)]
    pltpu.make_async_remote_copy(
        src_ref=others, dst_ref=others, send_sem=sum_send, recv_sem=sum_recv,
        device_id={"head": column(1)}, device_id_type=MESH,
    ).wait()
    line = jnp.sum(sums[...], axis=0)
    loss_ref[...] = line[:, :n_s] / (n_dp * rows * n_kv)


def finish(kl_in, loss_in, kl_ref, loss_ref):
    kl_ref[...] = kl_in[...]
    loss_ref[...] = loss_in[...]


def per_device(teacher_query, teacher_key, student_query, student_key, pair_table):
    n_dp, n_head, n_kv = lax.axis_size("dp"), lax.axis_size("head"), lax.axis_size("kv")
    seq_dev, rows, wide_t = teacher_query.shape
    assert seq_dev == 1
    n_t, n_s = HT // n_head, HS // n_head
    g_t, g_s = KVT // n_head, KVS // n_head
    n_rank = n_dp * n_head * n_kv
    pad = -(-n_s // 8) * 8
    key_t, key_s, query_s = g_t * DH, g_s * DH, n_s * DH
    spare = query_s + n_kv * key_s - (n_kv - 1) * (key_t + key_s)
    shared = min(max(round(spare / (2 * key_s * max(n_head - 1, 1))), 0), n_kv - 1)
    f32, bf16 = jnp.float32, jnp.bfloat16
    dma = pltpu.SemaphoreType.DMA
    kl, loss = pl.pallas_call(
        functools.partial(kernel, n_dp, n_head, n_kv, rows, shared),
        out_shape=(
            jax.ShapeDtypeStruct((n_s, 1, rows), f32),
            jax.ShapeDtypeStruct((1, n_s), f32),
        ),
        in_specs=[pl.BlockSpec(memory_space=pl.ANY)] * 5,
        out_specs=(
            pl.BlockSpec(memory_space=pltpu.VMEM),
            pl.BlockSpec(memory_space=pltpu.VMEM),
        ),
        scratch_shapes=[
            pltpu.VMEM((rows, wide_t), bf16),
            pltpu.VMEM((n_kv, rows, g_t * DH), bf16),
            pltpu.VMEM((n_head, rows, n_s * DH), bf16),
            pltpu.VMEM((n_head, n_kv, rows, g_s * DH), bf16),
            pltpu.VMEM((n_t, DH, rows), bf16),
            pltpu.VMEM((HS, DH, rows), bf16),
            pltpu.VMEM((g_t * KVS, 2 * DH + 16, rows), bf16),
            pltpu.VMEM((n_t, rows, rows), bf16),
            pltpu.VMEM((n_t, 2 * DH + 16, rows), f32),
            pltpu.VMEM((n_t, 1, rows), f32),
            pltpu.VMEM((n_t, 1, rows), f32),
            pltpu.VMEM((n_s, 1, rows), f32),
            pltpu.VMEM((n_s, 1, rows), f32),
            pltpu.SMEM(pair_table.shape[::-1], jnp.int32),
            pltpu.SMEM((n_t,), jnp.int32),
            pltpu.VMEM((n_head * pad, rows), f32),
            pltpu.VMEM((max(n_head - 1, 1), pad, rows), f32),
            pltpu.VMEM((n_head, 1, 128), f32),
            pltpu.VMEM((n_rank, 1, 128), f32),
            pltpu.SemaphoreType.REGULAR,
            pltpu.SemaphoreType.REGULAR((2,)),
            dma((5,)),
            dma((n_kv, max(n_head - 1, 1))),
            dma((n_kv, max(n_head - 1, 1))),
            dma((3, max(n_head - 1, 1))),
            dma((3, max(n_head - 1, 1))),
            dma((max(n_head - 1, 1),)),
            dma((max(n_head - 1, 1),)),
            dma((n_kv, n_head + 1)),
            dma((n_kv, n_head + 1)),
            dma(()),
            dma(()),
        ],
        compiler_params=pltpu.CompilerParams(collective_id=0, has_side_effects=True),
    )(pair_table.T, teacher_query, teacher_key, student_query, student_key)
    kl, loss = pl.pallas_call(
        finish,
        out_shape=(
            jax.ShapeDtypeStruct((n_s, 1, rows), f32),
            jax.ShapeDtypeStruct((1, n_s), f32),
        ),
        in_specs=[pl.BlockSpec(memory_space=pltpu.VMEM)] * 2,
        out_specs=(
            pl.BlockSpec(memory_space=pltpu.VMEM),
            pl.BlockSpec(memory_space=pltpu.VMEM),
        ),
    )(kl, loss)
    return kl.reshape(1, n_s, rows), loss.reshape(n_s)


def solution(mesh):
    split = P("dp", "kv", "head")
    return jax.shard_map(
        per_device,
        mesh=mesh,
        in_specs=(split, split, split, split, P()),
        out_specs=(P("dp", "head", "kv"), P("head")),
        check_vma=False,
    )
```

```python
import functools
import math

import jax
import jax.numpy as jnp
from jax import lax
from jax.experimental import pallas as pl
from jax.experimental.pallas import tpu as pltpu
from jax.sharding import PartitionSpec as P

HT = 28
KVT = 4
DH = 128
HS = 14
KVS = 2

MESH = pl.DeviceIdType.MESH
LOWEST = -1e30


def nn(a, b):
    return jnp.dot(a, b, preferred_element_type=jnp.float32)


def flip(x):
    n = x.shape[1]
    eye = (
        lax.broadcasted_iota(jnp.int32, (n, n), 0) == lax.broadcasted_iota(jnp.int32, (n, n), 1)
    ).astype(jnp.bfloat16)
    out = lax.dot_general(eye, x, (((1,), (1,)), ((), ())), preferred_element_type=jnp.float32)
    return out.astype(jnp.bfloat16)


def kernel(
    n_dp, n_head, n_kv, rows, shared,
    table_hbm, tq_hbm, tk_hbm, sq_hbm, sk_hbm,
    kl_ref, loss_ref,
    tq, tk, sq, sk,
    tq_t, sq_t, key_t, weights, mixed, t_max, t_decay, s_max, s_sum,
    table, inverse, acc, acc_in, sums_out, sums,
    layer_sem, chain_sem, load_sem, key_send, key_recv, query_send, query_recv,
    back_send, back_recv, z_send, z_recv, sum_send, sum_recv,
):
    n_t, n_s = HT // n_head, HS // n_head
    g_t, g_s = KVT // n_head, KVS // n_head
    per_t, per_s = HT // KVT, HS // KVS
    dp, hd, kv = lax.axis_index("dp"), lax.axis_index("head"), lax.axis_index("kv")
    n_rank = n_dp * n_head * n_kv
    rank = (dp * n_head + hd) * n_kv + kv
    scale = 1.0 / math.sqrt(DH)
    rate = scale * math.log2(math.e)
    bf16 = jnp.bfloat16

    loads = [
        pltpu.make_async_copy(sk_hbm.at[0], sk.at[hd, kv], load_sem.at[0]),
        pltpu.make_async_copy(tk_hbm.at[0], tk.at[kv], load_sem.at[1]),
        pltpu.make_async_copy(sq_hbm.at[0], sq.at[hd], load_sem.at[2]),
        pltpu.make_async_copy(table_hbm, table, load_sem.at[3]),
        pltpu.make_async_copy(tq_hbm.at[0], tq, load_sem.at[4]),
    ]
    for load in loads:
        load.start()

    first, last = kv == 0, kv == n_kv - 1
    not_first, not_last = kv > 0, kv < n_kv - 1
    barrier = pltpu.get_barrier_semaphore()

    def greet(sem, **peer):
        pl.semaphore_signal(sem, inc=1, device_id=peer, device_id_type=MESH)

    @pl.when(not_first)
    def _():
        greet(barrier, kv=kv - 1)

    @pl.when(not_last)
    def _():
        greet(barrier, kv=kv + 1)

    for s in range(1, n_head):
        greet(barrier, head=(hd + s) % n_head)
    for s in range(1, n_dp):
        greet(barrier, dp=(dp + s) % n_dp)

    def column(step):
        return (hd + step) % n_head

    def across(step, src, dst, send, recv):
        return pltpu.make_async_remote_copy(
            src_ref=src, dst_ref=dst, send_sem=send, recv_sem=recv,
            device_id={"head": column(step)}, device_id_type=MESH,
        )

    def keys_over(block):
        return [
            across(
                s, sk.at[hd, block], sk.at[hd, block],
                key_send.at[block, s - 1], key_recv.at[block, s - 1],
            )
            for s in range(1, n_head)
        ]

    cuts = [0, n_s * 2 // 7, n_s * 5 // 7, n_s]
    n_group = len(cuts) - 1

    def queries_over(group):
        part = sq.at[hd, :, cuts[group] * DH:cuts[group + 1] * DH]
        return [
            across(s, part, part, query_send.at[group, s - 1], query_recv.at[group, s - 1])
            for s in range(1, n_head)
        ]

    def start(copies):
        for copy in copies:
            copy.start()

    def upward(block, piece):
        ref = tk.at[block] if piece == n_head else sk.at[column(piece), block]
        return pltpu.make_async_remote_copy(
            src_ref=ref, dst_ref=ref, send_sem=z_send.at[block, piece],
            recv_sem=z_recv.at[block, piece],
            device_id={"kv": jnp.minimum(kv + 1, n_kv - 1)}, device_id_type=MESH,
        )

    def launch(block, piece):
        @pl.when(not_last)
        def _():
            upward(block, piece).start()

    def land(block, piece):
        upward(block, piece).wait_recv()
        launch(block, piece)

    def receive_own(block):
        @pl.when(block >= shared)
        def _():
            land(block, 0)
            start(keys_over(block))

    def receive_rest(block):
        land(block, n_head)

        @pl.when(block < shared)
        def _():
            land(block, 0)
            for s in range(1, n_head):
                land(block, s)

    loads[0].wait()
    loads[1].wait()
    pl.semaphore_wait(
        barrier, n_dp - 1 + n_head - 1 + not_first.astype(jnp.int32) + not_last.astype(jnp.int32)
    )
    start(keys_over(kv))

    @pl.when(kv < shared)
    def _():
        launch(kv, n_head)
        launch(kv, 0)

    @pl.when(kv >= shared)
    def _():
        launch(kv, 0)
        launch(kv, n_head)

    loads[2].wait()
    start(queries_over(0))
    for s in range(1, n_head):
        greet(layer_sem, head=column(s))

    loads[3].wait()
    entries = [table[k % 2, k // 2] for k in range(HT)]
    for t in range(n_t):
        found = jnp.int32(0)
        for k in range(HT):
            found = jnp.where(entries[k] == hd * n_t + t, k // 2, found)
        inverse[t] = found

    loads[4].wait()
    for h in range(n_t):
        tq_t[h] = flip(tq[:, h * DH:(h + 1) * DH])
    for h in range(n_s):
        sq_t[hd * n_s + h] = flip(sq[hd, :, h * DH:(h + 1) * DH])
    key_t[:, 2 * DH:] = jnp.ones((g_t * KVS, 16, rows), bf16)
    mixed[...] = jnp.zeros(mixed.shape, jnp.float32)

    pl.semaphore_wait(layer_sem, n_head - 1)
    for way, inner in ((0, not_last), (1, not_first)):
        @pl.when(not_first & not_last)
        def _():
            pl.semaphore_wait(chain_sem.at[way], 1)

        @pl.when(inner)
        def _():
            greet(chain_sem.at[way], kv=kv + 1 - 2 * way)

    @pl.when(kv < shared)
    def _():
        for copy in keys_over(kv):
            copy.wait_recv()
        for s in range(1, n_head):
            launch(kv, s)

    @pl.when(not_last & not_first)
    def _():
        receive_own(kv - 1)
        receive_rest(kv - 1)

    visible = lax.broadcasted_iota(jnp.int32, (rows, rows), 0) <= lax.broadcasted_iota(
        jnp.int32, (rows, rows), 1
    )

    def weigh(logits, high, row, diagonal):
        if diagonal:
            logits = jnp.where(visible, logits, LOWEST)
        top = jnp.max(logits, axis=0, keepdims=True)
        if diagonal:
            decay = jnp.zeros_like(top)
        else:
            old = high[row]
            top = jnp.maximum(old, top)
            decay = jnp.exp2((old - top) * rate)
        high[row] = top
        return jnp.exp2((logits - top) * rate), decay

    def turn_student(c, block):
        for j in range(g_s):
            flipped = flip(sk[c, block, :, j * DH:(j + 1) * DH])
            for g in range(g_t):
                key_t[g * KVS + c * g_s + j, DH:2 * DH] = flipped

    def weigh_block(block, diagonal):
        if not diagonal:
            @pl.when(last)
            def _():
                upward(block, n_head).wait_recv()

        for h in range(n_t):
            g = h // per_t
            logits = nn(tk[block, :, g * DH:(g + 1) * DH], tq_t[h])
            weight, t_decay[h] = weigh(logits, t_max, h, diagonal)
            weights[h] = weight.astype(bf16)
        for g in range(g_t):
            flipped = flip(tk[block, :, g * DH:(g + 1) * DH])
            for j in range(KVS):
                key_t[g * KVS + j, :DH] = flipped

        if not diagonal:
            @pl.when(last & (block < shared))
            def _():
                upward(block, 0).wait_recv()

        for h in range(n_s):
            g = h // per_s
            logits = nn(sk[hd, block, :, g * DH:(g + 1) * DH], sq_t[hd * n_s + h])
            weight, decay = weigh(logits, s_max, h, diagonal)
            part = jnp.sum(weight, axis=0, keepdims=True)
            s_sum[h] = part if diagonal else s_sum[h] * decay + part
        turn_student(hd, block)

    def await_others(block):
        @pl.when((block < shared) & last & not_first & (block != kv))
        def _():
            for s in range(1, n_head):
                upward(block, s).wait_recv()

        @pl.when(block >= shared)
        def _():
            for copy in keys_over(block):
                copy.wait_recv()

        for s in range(1, n_head):
            turn_student(column(s), block)

    def mix(h):
        part = nn(key_t[h // per_t * KVS + inverse[h] // per_s], weights[h])
        return mixed[h] * t_decay[h] + part

    def after_own():
        @pl.when(last & not_first)
        def _():
            receive_own(kv - 1)

        start(queries_over(1))

        @pl.when(first)
        def _():
            start(queries_over(2))

    weigh_block(kv, True)
    after_own()

    def step(s, carry):
        block = kv - s

        @pl.when(not_last & (s < kv))
        def _():
            receive_own(block - 1)
            receive_rest(block - 1)

        await_others(block + 1)
        for h in range(n_t):
            mixed[h] = mix(h)
        weigh_block(block, False)

        @pl.when(last & (s < kv))
        def _():
            receive_own(block - 1)

        @pl.when(s == 1)
        def _():
            start(queries_over(2))

        return carry

    lax.fori_loop(1, kv + 1, step, 0)

    for group in range(n_group):
        for copy in queries_over(group):
            copy.wait_recv()
        for s in range(1, n_head):
            for h in range(cuts[group], cuts[group + 1]):
                sq_t[column(s) * n_s + h] = flip(sq[column(s), :, h * DH:(h + 1) * DH])

    await_others(0)
    pad = acc.shape[0] // n_head
    place = lax.broadcasted_iota(jnp.int32, acc.shape, 0)
    total = jnp.zeros(acc.shape, jnp.float32)
    for h in range(n_t):
        partner = inverse[h]
        blend = mix(h)
        own = blend[:DH] * tq_t[h].astype(jnp.float32)
        other = blend[DH:2 * DH] * sq_t[partner].astype(jnp.float32)
        mass = blend[2 * DH:2 * DH + 1]
        value = jnp.sum(own - other, axis=0, keepdims=True) * scale / mass
        value = value - (t_max[h] * scale + jnp.log(mass))
        row = (partner // n_s) * pad + partner % n_s
        total = total + jnp.where(place == row, value, 0.0)
    acc[...] = total

    returns = [
        across(
            s, acc.at[pl.ds(column(s) * pad, pad)], acc_in.at[s - 1],
            back_send.at[s - 1], back_recv.at[s - 1],
        )
        for s in range(1, n_head)
    ]
    start(returns)
    lse = jnp.concatenate(
        [s_max[h] * scale + jnp.log(s_sum[h]) for h in range(n_s)]
        + [jnp.zeros((1, rows), jnp.float32)] * (pad - n_s),
        axis=0,
    )
    mine = jnp.where(place // pad == hd, 2.0 * jnp.concatenate([lse] * n_head, axis=0), 0.0)
    side = jnp.sum(total + mine, axis=1, keepdims=True)
    across_lanes = lax.broadcasted_iota(jnp.int32, (n_head * pad, 128), 1)
    down_rows = lax.broadcasted_iota(jnp.int32, (n_head * pad, 128), 0)
    for d in range(n_head):
        sums_out[d] = jnp.sum(
            jnp.where(down_rows == across_lanes + d * pad, side, 0.0), axis=0, keepdims=True
        )

    def share(d, h, k):
        return pltpu.make_async_remote_copy(
            src_ref=sums_out.at[h], dst_ref=sums.at[rank],
            send_sem=sum_send, recv_sem=sum_recv,
            device_id=(d, h, k), device_id_type=MESH,
        )

    def each_peer(act):
        def outer(k, carry):
            def middle(d, carry):
                for h in range(n_head):
                    @pl.when((d * n_head + h) * n_kv + k != rank)
                    def _():
                        act(d, h, k)
                return carry
            return lax.fori_loop(0, n_dp, middle, carry)
        lax.fori_loop(0, n_kv, outer, 0)

    for way, edge in ((0, last), (1, first)):
        @pl.when(edge)
        def _():
            pl.semaphore_wait(chain_sem.at[way], 1)

    each_peer(lambda d, h, k: share(d, h, k).start())
    sums[rank] = sums_out[hd]
    kl = acc[pl.ds(hd * pad, pad)] + 2.0 * lse
    for s in range(1, n_head):
        returns[s - 1].wait()
        kl = kl + acc_in[s - 1]
    for h in range(n_s):
        kl_ref[h] = kl[h:h + 1]

    for group in range(n_group):
        for copy in queries_over(group):
            copy.wait_send()

    def drain(block, carry):
        @pl.when((block >= shared) | (block == kv))
        def _():
            for copy in keys_over(block):
                copy.wait_send()

        @pl.when(not_last)
        def _():
            upward(block, 0).wait_send()
            upward(block, n_head).wait_send()

            @pl.when(block < shared)
            def _():
                for s in range(1, n_head):
                    upward(block, s).wait_send()
        return carry

    lax.fori_loop(0, kv + 1, drain, 0)

    others = sums.at[pl.ds(0, n_rank - 1)]
    pltpu.make_async_remote_copy(
        src_ref=others, dst_ref=others, send_sem=sum_send, recv_sem=sum_recv,
        device_id={"head": column(1)}, device_id_type=MESH,
    ).wait()
    line = jnp.sum(sums[...], axis=0)
    loss_ref[...] = line[:, :n_s] / (n_dp * rows * n_kv)


def per_device(teacher_query, teacher_key, student_query, student_key, pair_table):
    n_dp, n_head, n_kv = lax.axis_size("dp"), lax.axis_size("head"), lax.axis_size("kv")
    seq_dev, rows, wide_t = teacher_query.shape
    assert seq_dev == 1
    n_t, n_s = HT // n_head, HS // n_head
    g_t, g_s = KVT // n_head, KVS // n_head
    n_rank = n_dp * n_head * n_kv
    pad = -(-n_s // 8) * 8
    key_t, key_s, query_s = g_t * DH, g_s * DH, n_s * DH
    spare = query_s + n_kv * key_s - (n_kv - 1) * (key_t + key_s)
    shared = min(max(round(spare / (2 * key_s * max(n_head - 1, 1))), 0), n_kv - 1)
    f32, bf16 = jnp.float32, jnp.bfloat16
    dma = pltpu.SemaphoreType.DMA
    kl, loss = pl.pallas_call(
        functools.partial(kernel, n_dp, n_head, n_kv, rows, shared),
        out_shape=(
            pltpu.VMEM((n_s, 1, rows), f32),
            pltpu.VMEM((1, n_s), f32),
        ),
        in_specs=[pl.BlockSpec(memory_space=pl.ANY)] * 5,
        out_specs=(
            pl.BlockSpec(memory_space=pltpu.VMEM),
            pl.BlockSpec(memory_space=pltpu.VMEM),
        ),
        scratch_shapes=[
            pltpu.VMEM((rows, wide_t), bf16),
            pltpu.VMEM((n_kv, rows, g_t * DH), bf16),
            pltpu.VMEM((n_head, rows, n_s * DH), bf16),
            pltpu.VMEM((n_head, n_kv, rows, g_s * DH), bf16),
            pltpu.VMEM((n_t, DH, rows), bf16),
            pltpu.VMEM((HS, DH, rows), bf16),
            pltpu.VMEM((g_t * KVS, 2 * DH + 16, rows), bf16),
            pltpu.VMEM((n_t, rows, rows), bf16),
            pltpu.VMEM((n_t, 2 * DH + 16, rows), f32),
            pltpu.VMEM((n_t, 1, rows), f32),
            pltpu.VMEM((n_t, 1, rows), f32),
            pltpu.VMEM((n_s, 1, rows), f32),
            pltpu.VMEM((n_s, 1, rows), f32),
            pltpu.SMEM(pair_table.shape[::-1], jnp.int32),
            pltpu.SMEM((n_t,), jnp.int32),
            pltpu.VMEM((n_head * pad, rows), f32),
            pltpu.VMEM((max(n_head - 1, 1), pad, rows), f32),
            pltpu.VMEM((n_head, 1, 128), f32),
            pltpu.VMEM((n_rank, 1, 128), f32),
            pltpu.SemaphoreType.REGULAR,
            pltpu.SemaphoreType.REGULAR((2,)),
            dma((5,)),
            dma((n_kv, max(n_head - 1, 1))),
            dma((n_kv, max(n_head - 1, 1))),
            dma((3, max(n_head - 1, 1))),
            dma((3, max(n_head - 1, 1))),
            dma((max(n_head - 1, 1),)),
            dma((max(n_head - 1, 1),)),
            dma((n_kv, n_head + 1)),
            dma((n_kv, n_head + 1)),
            dma(()),
            dma(()),
        ],
        compiler_params=pltpu.CompilerParams(collective_id=0, has_side_effects=True),
    )(pair_table.T, teacher_query, teacher_key, student_query, student_key)
    return kl.reshape(1, n_s, rows), loss.reshape(n_s)


def solution(mesh):
    split = P("dp", "kv", "head")
    return jax.shard_map(
        per_device,
        mesh=mesh,
        in_specs=(split, split, split, split, P()),
        out_specs=(P("dp", "head", "kv"), P("head")),
        check_vma=False,
    )
```

```python
import functools
import math

import jax
import jax.numpy as jnp
from jax import lax
from jax.experimental import pallas as pl
from jax.experimental.pallas import tpu as pltpu
from jax.sharding import PartitionSpec as P

HT = 28
KVT = 4
DH = 128
HS = 14
KVS = 2

MESH = pl.DeviceIdType.MESH
LOWEST = -1e30


def nn(a, b):
    return jnp.dot(a, b, preferred_element_type=jnp.float32)


def flip(x):
    n = x.shape[1]
    eye = (
        lax.broadcasted_iota(jnp.int32, (n, n), 0) == lax.broadcasted_iota(jnp.int32, (n, n), 1)
    ).astype(jnp.bfloat16)
    out = lax.dot_general(eye, x, (((1,), (1,)), ((), ())), preferred_element_type=jnp.float32)
    return out.astype(jnp.bfloat16)


def kernel(
    n_dp, n_head, n_kv, rows, shared,
    table_hbm, tq_hbm, tk_hbm, sq_hbm, sk_hbm,
    kl_ref, loss_ref,
    tq, tk, sq, sk,
    tq_t, sq_t, key_t, weights, mixed, t_max, t_decay, s_max, s_sum,
    table, inverse, acc, acc_in, sums_out, sums,
    layer_sem, chain_sem, load_sem, key_send, key_recv, query_send, query_recv,
    back_send, back_recv, z_send, z_recv, sum_send, sum_recv,
):
    n_t, n_s = HT // n_head, HS // n_head
    g_t, g_s = KVT // n_head, KVS // n_head
    per_t, per_s = HT // KVT, HS // KVS
    dp, hd, kv = lax.axis_index("dp"), lax.axis_index("head"), lax.axis_index("kv")
    n_rank = n_dp * n_head * n_kv
    rank = (dp * n_head + hd) * n_kv + kv
    scale = 1.0 / math.sqrt(DH)
    rate = scale * math.log2(math.e)
    bf16 = jnp.bfloat16

    loads = [
        pltpu.make_async_copy(sk_hbm.at[0], sk.at[hd, kv], load_sem.at[0]),
        pltpu.make_async_copy(tk_hbm.at[0], tk.at[kv], load_sem.at[1]),
        pltpu.make_async_copy(sq_hbm.at[0], sq.at[hd], load_sem.at[2]),
        pltpu.make_async_copy(table_hbm, table, load_sem.at[3]),
        pltpu.make_async_copy(tq_hbm.at[0], tq, load_sem.at[4]),
    ]
    for load in loads:
        load.start()

    first, last = kv == 0, kv == n_kv - 1
    not_first, not_last = kv > 0, kv < n_kv - 1
    barrier = pltpu.get_barrier_semaphore()

    def greet(sem, **peer):
        pl.semaphore_signal(sem, inc=1, device_id=peer, device_id_type=MESH)

    @pl.when(not_first)
    def _():
        greet(barrier, kv=kv - 1)

    @pl.when(not_last)
    def _():
        greet(barrier, kv=kv + 1)

    for s in range(1, n_head):
        greet(barrier, head=(hd + s) % n_head)
    for s in range(1, n_dp):
        greet(barrier, dp=(dp + s) % n_dp)

    def column(step):
        return (hd + step) % n_head

    def across(step, src, dst, send, recv):
        return pltpu.make_async_remote_copy(
            src_ref=src, dst_ref=dst, send_sem=send, recv_sem=recv,
            device_id={"head": column(step)}, device_id_type=MESH,
        )

    def keys_over(block):
        return [
            across(
                s, sk.at[hd, block], sk.at[hd, block],
                key_send.at[block, s - 1], key_recv.at[block, s - 1],
            )
            for s in range(1, n_head)
        ]

    cuts = [0, n_s * 2 // 7, n_s * 5 // 7, n_s]
    n_group = len(cuts) - 1

    def queries_over(group):
        part = sq.at[hd, :, cuts[group] * DH:cuts[group + 1] * DH]
        return [
            across(s, part, part, query_send.at[group, s - 1], query_recv.at[group, s - 1])
            for s in range(1, n_head)
        ]

    def start(copies):
        for copy in copies:
            copy.start()

    half = rows // 2
    halves = (n_head, n_head + 1)

    def upward(block, piece):
        if piece < n_head:
            ref = sk.at[column(piece), block]
        else:
            ref = tk.at[block, pl.ds((piece - n_head) * half, half)]
        return pltpu.make_async_remote_copy(
            src_ref=ref, dst_ref=ref, send_sem=z_send.at[block, piece],
            recv_sem=z_recv.at[block, piece],
            device_id={"kv": jnp.minimum(kv + 1, n_kv - 1)}, device_id_type=MESH,
        )

    def launch(block, piece):
        @pl.when(not_last)
        def _():
            upward(block, piece).start()

    def land(block, piece):
        upward(block, piece).wait_recv()
        launch(block, piece)

    def receive_own(block):
        @pl.when(block >= shared)
        def _():
            land(block, 0)
            start(keys_over(block))

    def receive_rest(block):
        for piece in halves:
            land(block, piece)

        @pl.when(block < shared)
        def _():
            land(block, 0)
            for s in range(1, n_head):
                land(block, s)

    loads[0].wait()
    pl.semaphore_wait(
        barrier, n_dp - 1 + n_head - 1 + not_first.astype(jnp.int32) + not_last.astype(jnp.int32)
    )
    start(keys_over(kv))

    @pl.when(kv < shared)
    def _():
        loads[1].wait()
        for piece in halves:
            launch(kv, piece)
        launch(kv, 0)

    @pl.when(kv >= shared)
    def _():
        launch(kv, 0)
        loads[1].wait()
        for piece in halves:
            launch(kv, piece)

    loads[2].wait()
    start(queries_over(0))
    for s in range(1, n_head):
        greet(layer_sem, head=column(s))

    loads[3].wait()
    entries = [table[k % 2, k // 2] for k in range(HT)]
    for t in range(n_t):
        found = jnp.int32(0)
        for k in range(HT):
            found = jnp.where(entries[k] == hd * n_t + t, k // 2, found)
        inverse[t] = found

    loads[4].wait()
    for h in range(n_t):
        tq_t[h] = flip(tq[:, h * DH:(h + 1) * DH])
    for h in range(n_s):
        sq_t[hd * n_s + h] = flip(sq[hd, :, h * DH:(h + 1) * DH])
    key_t[:, :, 2 * DH:] = jnp.ones((2, g_t * KVS, 16, rows), bf16)
    mixed[...] = jnp.zeros(mixed.shape, jnp.float32)

    pl.semaphore_wait(layer_sem, n_head - 1)
    for way, inner in ((0, not_last), (1, not_first)):
        @pl.when(not_first & not_last)
        def _():
            pl.semaphore_wait(chain_sem.at[way], 1)

        @pl.when(inner)
        def _():
            greet(chain_sem.at[way], kv=kv + 1 - 2 * way)

    @pl.when(kv < shared)
    def _():
        for copy in keys_over(kv):
            copy.wait_recv()
        for s in range(1, n_head):
            launch(kv, s)

    @pl.when(not_last & not_first)
    def _():
        receive_own(kv - 1)
        receive_rest(kv - 1)

    visible = lax.broadcasted_iota(jnp.int32, (rows, rows), 0) <= lax.broadcasted_iota(
        jnp.int32, (rows, rows), 1
    )

    def weigh(logits, high, row, diagonal):
        if diagonal:
            logits = jnp.where(visible, logits, LOWEST)
        top = jnp.max(logits, axis=0, keepdims=True)
        if diagonal:
            decay = jnp.zeros_like(top)
        else:
            old = high[row]
            top = jnp.maximum(old, top)
            decay = jnp.exp2((old - top) * rate)
        high[row] = top
        return jnp.exp2((logits - top) * rate), decay

    def turn_student(c, block, slot):
        for j in range(g_s):
            flipped = flip(sk[c, block, :, j * DH:(j + 1) * DH])
            for g in range(g_t):
                key_t[slot, g * KVS + c * g_s + j, DH:2 * DH] = flipped

    def weigh_block(block, slot, diagonal):
        if not diagonal:
            @pl.when(last)
            def _():
                for piece in halves:
                    upward(block, piece).wait_recv()

        for h in range(n_t):
            g = h // per_t
            logits = nn(tk[block, :, g * DH:(g + 1) * DH], tq_t[h])
            weight, t_decay[slot, h] = weigh(logits, t_max, h, diagonal)
            weights[slot, h] = weight.astype(bf16)
        for g in range(g_t):
            flipped = flip(tk[block, :, g * DH:(g + 1) * DH])
            for j in range(KVS):
                key_t[slot, g * KVS + j, :DH] = flipped

        if not diagonal:
            @pl.when(last & (block < shared))
            def _():
                upward(block, 0).wait_recv()

        for h in range(n_s):
            g = h // per_s
            logits = nn(sk[hd, block, :, g * DH:(g + 1) * DH], sq_t[hd * n_s + h])
            weight, decay = weigh(logits, s_max, h, diagonal)
            part = jnp.sum(weight, axis=0, keepdims=True)
            s_sum[h] = part if diagonal else s_sum[h] * decay + part
        turn_student(hd, block, slot)

    def await_others(block, slot):
        @pl.when((block < shared) & last & not_first & (block != kv))
        def _():
            for s in range(1, n_head):
                upward(block, s).wait_recv()

        @pl.when(block >= shared)
        def _():
            for copy in keys_over(block):
                copy.wait_recv()

        for s in range(1, n_head):
            turn_student(column(s), block, slot)

    def mix(h, slot):
        part = nn(key_t[slot, h // per_t * KVS + inverse[h] // per_s], weights[slot, h])
        return mixed[h] * t_decay[slot, h] + part

    def turn_queries(groups):
        for group in groups:
            for copy in queries_over(group):
                copy.wait_recv()
            for s in range(1, n_head):
                for h in range(cuts[group], cuts[group + 1]):
                    sq_t[column(s) * n_s + h] = flip(sq[column(s), :, h * DH:(h + 1) * DH])

    def after_own():
        @pl.when(last & not_first)
        def _():
            receive_own(kv - 1)

        start(queries_over(1))

        @pl.when(first)
        def _():
            start(queries_over(2))

    weigh_block(kv, 0, True)
    after_own()

    def step(s, carry):
        block = kv - s

        @pl.when(not_last & (s < kv))
        def _():
            receive_own(block - 1)
            receive_rest(block - 1)

        @pl.when((s == kv) & (s > 1))
        def _():
            turn_queries((0, 1))

        weigh_block(block, s % 2, False)

        @pl.when(last & (s < kv))
        def _():
            receive_own(block - 1)

        @pl.when(s == 1)
        def _():
            start(queries_over(2))

        await_others(block + 1, (s - 1) % 2)
        for h in range(n_t):
            mixed[h] = mix(h, (s - 1) % 2)
        return carry

    lax.fori_loop(1, kv + 1, step, 0)

    @pl.when(kv <= 1)
    def _():
        turn_queries((0, 1))

    pad = acc.shape[0] // n_head
    place = lax.broadcasted_iota(jnp.int32, acc.shape, 0)
    lse = jnp.concatenate(
        [s_max[h] * scale + jnp.log(s_sum[h]) for h in range(n_s)]
        + [jnp.zeros((1, rows), jnp.float32)] * (pad - n_s),
        axis=0,
    )
    mine = jnp.where(place // pad == hd, 2.0 * jnp.concatenate([lse] * n_head, axis=0), 0.0)
    turn_queries((2,))
    await_others(0, kv % 2)
    total = jnp.zeros(acc.shape, jnp.float32)
    for h in range(n_t):
        partner = inverse[h]
        blend = mix(h, kv % 2)
        own = blend[:DH] * tq_t[h].astype(jnp.float32)
        other = blend[DH:2 * DH] * sq_t[partner].astype(jnp.float32)
        mass = blend[2 * DH:2 * DH + 1]
        value = jnp.sum(own - other, axis=0, keepdims=True) * scale / mass
        value = value - (t_max[h] * scale + jnp.log(mass))
        row = (partner // n_s) * pad + partner % n_s
        total = total + jnp.where(place == row, value, 0.0)
    acc[...] = total

    returns = [
        across(
            s, acc.at[pl.ds(column(s) * pad, pad)], acc_in.at[s - 1],
            back_send.at[s - 1], back_recv.at[s - 1],
        )
        for s in range(1, n_head)
    ]
    start(returns)
    side = jnp.sum(total + mine, axis=1, keepdims=True)
    across_lanes = lax.broadcasted_iota(jnp.int32, (n_head * pad, 128), 1)
    down_rows = lax.broadcasted_iota(jnp.int32, (n_head * pad, 128), 0)
    for d in range(n_head):
        sums_out[d] = jnp.sum(
            jnp.where(down_rows == across_lanes + d * pad, side, 0.0), axis=0, keepdims=True
        )

    def share(d, h, k):
        return pltpu.make_async_remote_copy(
            src_ref=sums_out.at[h], dst_ref=sums.at[rank],
            send_sem=sum_send, recv_sem=sum_recv,
            device_id=(d, h, k), device_id_type=MESH,
        )

    def each_peer(act):
        def outer(k, carry):
            def middle(d, carry):
                for h in range(n_head):
                    @pl.when((d * n_head + h) * n_kv + k != rank)
                    def _():
                        act(d, h, k)
                return carry
            return lax.fori_loop(0, n_dp, middle, carry)
        lax.fori_loop(0, n_kv, outer, 0)

    for way, edge in ((0, last), (1, first)):
        @pl.when(edge)
        def _():
            pl.semaphore_wait(chain_sem.at[way], 1)

    each_peer(lambda d, h, k: share(d, h, k).start())
    sums[rank] = sums_out[hd]
    kl = acc[pl.ds(hd * pad, pad)] + 2.0 * lse
    for s in range(1, n_head):
        returns[s - 1].wait()
        kl = kl + acc_in[s - 1]
    for h in range(n_s):
        kl_ref[h] = kl[h:h + 1]

    for group in range(n_group):
        for copy in queries_over(group):
            copy.wait_send()

    def drain(block, carry):
        @pl.when((block >= shared) | (block == kv))
        def _():
            for copy in keys_over(block):
                copy.wait_send()

        @pl.when(not_last)
        def _():
            upward(block, 0).wait_send()
            for piece in halves:
                upward(block, piece).wait_send()

            @pl.when(block < shared)
            def _():
                for s in range(1, n_head):
                    upward(block, s).wait_send()
        return carry

    lax.fori_loop(0, kv + 1, drain, 0)

    others = sums.at[pl.ds(0, n_rank - 1)]
    pltpu.make_async_remote_copy(
        src_ref=others, dst_ref=others, send_sem=sum_send, recv_sem=sum_recv,
        device_id={"head": column(1)}, device_id_type=MESH,
    ).wait()
    line = jnp.sum(sums[...], axis=0)
    loss_ref[...] = line[:, :n_s] / (n_dp * rows * n_kv)


def finish(kl_in, loss_in, kl_ref, loss_ref):
    kl_ref[...] = kl_in[...]
    loss_ref[...] = loss_in[...]


def per_device(teacher_query, teacher_key, student_query, student_key, pair_table):
    n_dp, n_head, n_kv = lax.axis_size("dp"), lax.axis_size("head"), lax.axis_size("kv")
    seq_dev, rows, wide_t = teacher_query.shape
    assert seq_dev == 1
    n_t, n_s = HT // n_head, HS // n_head
    g_t, g_s = KVT // n_head, KVS // n_head
    n_rank = n_dp * n_head * n_kv
    pad = -(-n_s // 8) * 8
    key_t, key_s, query_s = g_t * DH, g_s * DH, n_s * DH
    spare = query_s + n_kv * key_s - (n_kv - 1) * (key_t + key_s)
    shared = min(max(round(spare / (2 * key_s * max(n_head - 1, 1))), 0), n_kv - 1)
    f32, bf16 = jnp.float32, jnp.bfloat16
    dma = pltpu.SemaphoreType.DMA
    kl, loss = pl.pallas_call(
        functools.partial(kernel, n_dp, n_head, n_kv, rows, shared),
        out_shape=(
            pltpu.VMEM((n_s, 1, rows), f32),
            pltpu.VMEM((1, n_s), f32),
        ),
        in_specs=[pl.BlockSpec(memory_space=pl.ANY)] * 5,
        out_specs=(
            pl.BlockSpec(memory_space=pltpu.VMEM),
            pl.BlockSpec(memory_space=pltpu.VMEM),
        ),
        scratch_shapes=[
            pltpu.VMEM((rows, wide_t), bf16),
            pltpu.VMEM((n_kv, rows, g_t * DH), bf16),
            pltpu.VMEM((n_head, rows, n_s * DH), bf16),
            pltpu.VMEM((n_head, n_kv, rows, g_s * DH), bf16),
            pltpu.VMEM((n_t, DH, rows), bf16),
            pltpu.VMEM((HS, DH, rows), bf16),
            pltpu.VMEM((2, g_t * KVS, 2 * DH + 16, rows), bf16),
            pltpu.VMEM((2, n_t, rows, rows), bf16),
            pltpu.VMEM((n_t, 2 * DH + 16, rows), f32),
            pltpu.VMEM((n_t, 1, rows), f32),
            pltpu.VMEM((2, n_t, 1, rows), f32),
            pltpu.VMEM((n_s, 1, rows), f32),
            pltpu.VMEM((n_s, 1, rows), f32),
            pltpu.SMEM(pair_table.shape[::-1], jnp.int32),
            pltpu.SMEM((n_t,), jnp.int32),
            pltpu.VMEM((n_head * pad, rows), f32),
            pltpu.VMEM((max(n_head - 1, 1), pad, rows), f32),
            pltpu.VMEM((n_head, 1, 128), f32),
            pltpu.VMEM((n_rank, 1, 128), f32),
            pltpu.SemaphoreType.REGULAR,
            pltpu.SemaphoreType.REGULAR((2,)),
            dma((5,)),
            dma((n_kv, max(n_head - 1, 1))),
            dma((n_kv, max(n_head - 1, 1))),
            dma((3, max(n_head - 1, 1))),
            dma((3, max(n_head - 1, 1))),
            dma((max(n_head - 1, 1),)),
            dma((max(n_head - 1, 1),)),
            dma((n_kv, n_head + 2)),
            dma((n_kv, n_head + 2)),
            dma(()),
            dma(()),
        ],
        compiler_params=pltpu.CompilerParams(collective_id=0, has_side_effects=True),
    )(pair_table.T, teacher_query, teacher_key, student_query, student_key)
    kl, loss = pl.pallas_call(
        finish,
        out_shape=(
            jax.ShapeDtypeStruct((n_s, 1, rows), f32),
            jax.ShapeDtypeStruct((1, n_s), f32),
        ),
        in_specs=[pl.BlockSpec(memory_space=pltpu.VMEM)] * 2,
        out_specs=(
            pl.BlockSpec(memory_space=pltpu.VMEM),
            pl.BlockSpec(memory_space=pltpu.VMEM),
        ),
    )(pltpu.with_memory_space_constraint(kl, pltpu.VMEM), pltpu.with_memory_space_constraint(loss, pltpu.VMEM))
    return kl.reshape(1, n_s, rows), loss.reshape(n_s)


def solution(mesh):
    split = P("dp", "kv", "head")
    return jax.shard_map(
        per_device,
        mesh=mesh,
        in_specs=(split, split, split, split, P()),
        out_specs=(P("dp", "head", "kv"), P("head")),
        check_vma=False,
    )
```

```python
import functools
import math

import jax
import jax.numpy as jnp
from jax import lax
from jax.experimental import pallas as pl
from jax.experimental.pallas import tpu as pltpu
from jax.sharding import PartitionSpec as P

HT = 28
KVT = 4
DH = 128
HS = 14
KVS = 2

MESH = pl.DeviceIdType.MESH
LOWEST = -1e30


def nn(a, b):
    return jnp.dot(a, b, preferred_element_type=jnp.float32)


def flip(x):
    n = x.shape[1]
    eye = (
        lax.broadcasted_iota(jnp.int32, (n, n), 0) == lax.broadcasted_iota(jnp.int32, (n, n), 1)
    ).astype(jnp.bfloat16)
    out = lax.dot_general(eye, x, (((1,), (1,)), ((), ())), preferred_element_type=jnp.float32)
    return out.astype(jnp.bfloat16)


def kernel(
    n_dp, n_head, n_kv, rows, shared,
    table_hbm, tq_hbm, tk_hbm, sq_hbm, sk_hbm,
    kl_ref, loss_ref,
    tq, tk, sq, sk,
    tq_t, sq_t, key_t, weights, mixed, t_max, t_decay, s_max, s_sum,
    table, inverse, acc, acc_in, sums_out, sums,
    layer_sem, chain_sem, load_sem, key_send, key_recv, query_send, query_recv,
    back_send, back_recv, z_send, z_recv, sum_send, sum_recv,
):
    n_t, n_s = HT // n_head, HS // n_head
    g_t, g_s = KVT // n_head, KVS // n_head
    per_t, per_s = HT // KVT, HS // KVS
    dp, hd, kv = lax.axis_index("dp"), lax.axis_index("head"), lax.axis_index("kv")
    n_rank = n_dp * n_head * n_kv
    rank = (dp * n_head + hd) * n_kv + kv
    scale = 1.0 / math.sqrt(DH)
    rate = scale * math.log2(math.e)
    bf16 = jnp.bfloat16

    loads = [
        pltpu.make_async_copy(sk_hbm.at[0], sk.at[hd, kv], load_sem.at[0]),
        pltpu.make_async_copy(tk_hbm.at[0], tk.at[kv], load_sem.at[1]),
        pltpu.make_async_copy(sq_hbm.at[0], sq.at[hd], load_sem.at[2]),
        pltpu.make_async_copy(table_hbm, table, load_sem.at[3]),
        pltpu.make_async_copy(tq_hbm.at[0], tq, load_sem.at[4]),
    ]
    for load in loads:
        load.start()

    first, last = kv == 0, kv == n_kv - 1
    not_first, not_last = kv > 0, kv < n_kv - 1
    barrier = pltpu.get_barrier_semaphore()

    def greet(sem, **peer):
        pl.semaphore_signal(sem, inc=1, device_id=peer, device_id_type=MESH)

    @pl.when(not_first)
    def _():
        greet(barrier, kv=kv - 1)

    @pl.when(not_last)
    def _():
        greet(barrier, kv=kv + 1)

    for s in range(1, n_head):
        greet(barrier, head=(hd + s) % n_head)
    for s in range(1, n_dp):
        greet(barrier, dp=(dp + s) % n_dp)

    def column(step):
        return (hd + step) % n_head

    def across(step, src, dst, send, recv):
        return pltpu.make_async_remote_copy(
            src_ref=src, dst_ref=dst, send_sem=send, recv_sem=recv,
            device_id={"head": column(step)}, device_id_type=MESH,
        )

    def keys_over(block):
        return [
            across(
                s, sk.at[hd, block], sk.at[hd, block],
                key_send.at[block, s - 1], key_recv.at[block, s - 1],
            )
            for s in range(1, n_head)
        ]

    cuts = [0, n_s * 2 // 7, n_s * 5 // 7, n_s]
    n_group = len(cuts) - 1

    def queries_over(group):
        part = sq.at[hd, :, cuts[group] * DH:cuts[group + 1] * DH]
        return [
            across(s, part, part, query_send.at[group, s - 1], query_recv.at[group, s - 1])
            for s in range(1, n_head)
        ]

    def start(copies):
        for copy in copies:
            copy.start()

    half = rows // 2
    halves = (n_head, n_head + 1)

    def upward(block, piece):
        if piece < n_head:
            ref = sk.at[column(piece), block]
        else:
            ref = tk.at[block, pl.ds((piece - n_head) * half, half)]
        return pltpu.make_async_remote_copy(
            src_ref=ref, dst_ref=ref, send_sem=z_send.at[block, piece],
            recv_sem=z_recv.at[block, piece],
            device_id={"kv": jnp.minimum(kv + 1, n_kv - 1)}, device_id_type=MESH,
        )

    def launch(block, piece):
        @pl.when(not_last)
        def _():
            upward(block, piece).start()

    def land(block, piece):
        upward(block, piece).wait_recv()
        launch(block, piece)

    def receive_own(block):
        @pl.when(block >= shared)
        def _():
            land(block, 0)
            start(keys_over(block))

    def receive_teacher(block):
        for piece in halves:
            land(block, piece)

    def receive_student(block):
        @pl.when(block < shared)
        def _():
            land(block, 0)
            for s in range(1, n_head):
                land(block, s)

    loads[0].wait()
    pl.semaphore_wait(
        barrier, n_dp - 1 + n_head - 1 + not_first.astype(jnp.int32) + not_last.astype(jnp.int32)
    )
    start(keys_over(kv))

    @pl.when(kv < shared)
    def _():
        loads[1].wait()
        for piece in halves:
            launch(kv, piece)
        launch(kv, 0)

    @pl.when(kv >= shared)
    def _():
        launch(kv, 0)
        loads[1].wait()
        for piece in halves:
            launch(kv, piece)

    loads[2].wait()
    start(queries_over(0))

    @pl.when(not_last)
    def _():
        start(queries_over(1))
        start(queries_over(2))

    for s in range(1, n_head):
        greet(layer_sem, head=column(s))

    loads[3].wait()
    entries = [table[k % 2, k // 2] for k in range(HT)]
    for t in range(n_t):
        found = jnp.int32(0)
        for k in range(HT):
            found = jnp.where(entries[k] == hd * n_t + t, k // 2, found)
        inverse[t] = found

    loads[4].wait()
    for h in range(n_t):
        tq_t[h] = flip(tq[:, h * DH:(h + 1) * DH])
    for h in range(n_s):
        sq_t[hd * n_s + h] = flip(sq[hd, :, h * DH:(h + 1) * DH])
    key_t[:, :, 2 * DH:] = jnp.ones((2, g_t * KVS, 16, rows), bf16)
    mixed[...] = jnp.zeros(mixed.shape, jnp.float32)

    pl.semaphore_wait(layer_sem, n_head - 1)
    for way, inner in ((0, not_last), (1, not_first)):
        @pl.when(not_first & not_last)
        def _():
            pl.semaphore_wait(chain_sem.at[way], 1)

        @pl.when(inner)
        def _():
            greet(chain_sem.at[way], kv=kv + 1 - 2 * way)

    @pl.when(kv < shared)
    def _():
        for copy in keys_over(kv):
            copy.wait_recv()
        for s in range(1, n_head):
            launch(kv, s)

    @pl.when(not_last & not_first)
    def _():
        receive_own(kv - 1)
        receive_teacher(kv - 1)
        receive_student(kv - 1)

    visible = lax.broadcasted_iota(jnp.int32, (rows, rows), 0) <= lax.broadcasted_iota(
        jnp.int32, (rows, rows), 1
    )

    def weigh(logits, high, row, diagonal):
        if diagonal:
            logits = jnp.where(visible, logits, LOWEST)
        top = jnp.max(logits, axis=0, keepdims=True)
        if diagonal:
            decay = jnp.zeros_like(top)
        else:
            old = high[row]
            top = jnp.maximum(old, top)
            decay = jnp.exp2((old - top) * rate)
        high[row] = top
        return jnp.exp2((logits - top) * rate), decay

    def turn_student(c, block, slot):
        for j in range(g_s):
            flipped = flip(sk[c, block, :, j * DH:(j + 1) * DH])
            for g in range(g_t):
                key_t[slot, g * KVS + c * g_s + j, DH:2 * DH] = flipped

    def weigh_block(block, slot, diagonal):
        if not diagonal:
            @pl.when(last)
            def _():
                for piece in halves:
                    upward(block, piece).wait_recv()

        for h in range(n_t):
            g = h // per_t
            logits = nn(tk[block, :, g * DH:(g + 1) * DH], tq_t[h])
            weight, t_decay[slot, h] = weigh(logits, t_max, h, diagonal)
            weights[slot, h] = weight.astype(bf16)
        for g in range(g_t):
            flipped = flip(tk[block, :, g * DH:(g + 1) * DH])
            for j in range(KVS):
                key_t[slot, g * KVS + j, :DH] = flipped

        if not diagonal:
            @pl.when(last & (block < shared))
            def _():
                upward(block, 0).wait_recv()

        for h in range(n_s):
            g = h // per_s
            logits = nn(sk[hd, block, :, g * DH:(g + 1) * DH], sq_t[hd * n_s + h])
            weight, decay = weigh(logits, s_max, h, diagonal)
            part = jnp.sum(weight, axis=0, keepdims=True)
            s_sum[h] = part if diagonal else s_sum[h] * decay + part
        turn_student(hd, block, slot)

    def await_others(block, slot):
        @pl.when((block < shared) & last & not_first & (block != kv))
        def _():
            for s in range(1, n_head):
                upward(block, s).wait_recv()

        @pl.when(block >= shared)
        def _():
            for copy in keys_over(block):
                copy.wait_recv()

        for s in range(1, n_head):
            turn_student(column(s), block, slot)

    def mix(h, slot):
        part = nn(key_t[slot, h // per_t * KVS + inverse[h] // per_s], weights[slot, h])
        return mixed[h] * t_decay[slot, h] + part

    def turn_queries(groups):
        for group in groups:
            for copy in queries_over(group):
                copy.wait_recv()
            for s in range(1, n_head):
                for h in range(cuts[group], cuts[group + 1]):
                    sq_t[column(s) * n_s + h] = flip(sq[column(s), :, h * DH:(h + 1) * DH])

    def after_own():
        @pl.when(last & not_first)
        def _():
            receive_own(kv - 1)

        @pl.when(last)
        def _():
            start(queries_over(1))

        @pl.when(last & first)
        def _():
            start(queries_over(2))

    weigh_block(kv, 0, True)
    after_own()

    def blend_before(s):
        await_others(kv - s + 1, (s - 1) % 2)
        for h in range(n_t):
            mixed[h] = mix(h, (s - 1) % 2)

    def step(s, carry):
        block = kv - s

        @pl.when(not_last & (s < kv))
        def _():
            receive_own(block - 1)
            receive_teacher(block - 1)

        @pl.when(s < kv)
        def _():
            blend_before(s)

        @pl.when(not_last & (s < kv))
        def _():
            receive_student(block - 1)

        @pl.when(s == kv - 1)
        def _():
            turn_queries((0,))

        @pl.when((s == kv) & (s > 1))
        def _():
            turn_queries((1,))

        weigh_block(block, s % 2, False)

        @pl.when(last & (s < kv))
        def _():
            receive_own(block - 1)

        @pl.when(last & (s == 1))
        def _():
            start(queries_over(2))

        @pl.when(s == kv)
        def _():
            blend_before(s)

        return carry

    lax.fori_loop(1, kv + 1, step, 0)

    @pl.when(kv <= 1)
    def _():
        turn_queries((0, 1))

    pad = acc.shape[0] // n_head
    place = lax.broadcasted_iota(jnp.int32, acc.shape, 0)
    lse = jnp.concatenate(
        [s_max[h] * scale + jnp.log(s_sum[h]) for h in range(n_s)]
        + [jnp.zeros((1, rows), jnp.float32)] * (pad - n_s),
        axis=0,
    )
    mine = jnp.where(place // pad == hd, 2.0 * jnp.concatenate([lse] * n_head, axis=0), 0.0)
    turn_queries((2,))
    await_others(0, kv % 2)
    total = jnp.zeros(acc.shape, jnp.float32)
    for h in range(n_t):
        partner = inverse[h]
        blend = mix(h, kv % 2)
        own = blend[:DH] * tq_t[h].astype(jnp.float32)
        other = blend[DH:2 * DH] * sq_t[partner].astype(jnp.float32)
        mass = blend[2 * DH:2 * DH + 1]
        value = jnp.sum(own - other, axis=0, keepdims=True) * scale / mass
        value = value - (t_max[h] * scale + jnp.log(mass))
        row = (partner // n_s) * pad + partner % n_s
        total = total + jnp.where(place == row, value, 0.0)
    acc[...] = total

    returns = [
        across(
            s, acc.at[pl.ds(column(s) * pad, pad)], acc_in.at[s - 1],
            back_send.at[s - 1], back_recv.at[s - 1],
        )
        for s in range(1, n_head)
    ]
    start(returns)
    side = jnp.sum(total + mine, axis=1, keepdims=True)
    across_lanes = lax.broadcasted_iota(jnp.int32, (n_head * pad, 128), 1)
    down_rows = lax.broadcasted_iota(jnp.int32, (n_head * pad, 128), 0)
    for d in range(n_head):
        sums_out[d] = jnp.sum(
            jnp.where(down_rows == across_lanes + d * pad, side, 0.0), axis=0, keepdims=True
        )

    def share(d, h, k):
        return pltpu.make_async_remote_copy(
            src_ref=sums_out.at[h], dst_ref=sums.at[rank],
            send_sem=sum_send, recv_sem=sum_recv,
            device_id=(d, h, k), device_id_type=MESH,
        )

    def each_peer(act):
        def outer(k, carry):
            def middle(d, carry):
                for h in range(n_head):
                    @pl.when((d * n_head + h) * n_kv + k != rank)
                    def _():
                        act(d, h, k)
                return carry
            return lax.fori_loop(0, n_dp, middle, carry)
        lax.fori_loop(0, n_kv, outer, 0)

    for way, edge in ((0, last), (1, first)):
        @pl.when(edge)
        def _():
            pl.semaphore_wait(chain_sem.at[way], 1)

    each_peer(lambda d, h, k: share(d, h, k).start())
    sums[rank] = sums_out[hd]
    kl = acc[pl.ds(hd * pad, pad)] + 2.0 * lse
    for s in range(1, n_head):
        returns[s - 1].wait()
        kl = kl + acc_in[s - 1]
    for h in range(n_s):
        kl_ref[h] = kl[h:h + 1]

    for group in range(n_group):
        for copy in queries_over(group):
            copy.wait_send()

    def drain(block, carry):
        @pl.when((block >= shared) | (block == kv))
        def _():
            for copy in keys_over(block):
                copy.wait_send()

        @pl.when(not_last)
        def _():
            upward(block, 0).wait_send()
            for piece in halves:
                upward(block, piece).wait_send()

            @pl.when(block < shared)
            def _():
                for s in range(1, n_head):
                    upward(block, s).wait_send()
        return carry

    lax.fori_loop(0, kv + 1, drain, 0)

    others = sums.at[pl.ds(0, n_rank - 1)]
    pltpu.make_async_remote_copy(
        src_ref=others, dst_ref=others, send_sem=sum_send, recv_sem=sum_recv,
        device_id={"head": column(1)}, device_id_type=MESH,
    ).wait()
    line = jnp.sum(sums[...], axis=0)
    loss_ref[...] = line[:, :n_s] * (1.0 / (n_dp * rows * n_kv))


def finish(kl_in, loss_in, kl_ref, loss_ref):
    kl_ref[...] = kl_in[...]
    loss_ref[...] = loss_in[...]


def per_device(teacher_query, teacher_key, student_query, student_key, pair_table):
    n_dp, n_head, n_kv = lax.axis_size("dp"), lax.axis_size("head"), lax.axis_size("kv")
    seq_dev, rows, wide_t = teacher_query.shape
    assert seq_dev == 1
    n_t, n_s = HT // n_head, HS // n_head
    g_t, g_s = KVT // n_head, KVS // n_head
    n_rank = n_dp * n_head * n_kv
    pad = -(-n_s // 8) * 8
    key_t, key_s, query_s = g_t * DH, g_s * DH, n_s * DH
    spare = query_s + n_kv * key_s - (n_kv - 1) * (key_t + key_s)
    shared = min(max(round(spare / (2 * key_s * max(n_head - 1, 1))), 0), n_kv - 1)
    f32, bf16 = jnp.float32, jnp.bfloat16
    dma = pltpu.SemaphoreType.DMA
    kl, loss = pl.pallas_call(
        functools.partial(kernel, n_dp, n_head, n_kv, rows, shared),
        out_shape=(
            pltpu.VMEM((n_s, 1, rows), f32),
            pltpu.VMEM((1, n_s), f32),
        ),
        in_specs=[pl.BlockSpec(memory_space=pl.ANY)] * 5,
        out_specs=(
            pl.BlockSpec(memory_space=pltpu.VMEM),
            pl.BlockSpec(memory_space=pltpu.VMEM),
        ),
        scratch_shapes=[
            pltpu.VMEM((rows, wide_t), bf16),
            pltpu.VMEM((n_kv, rows, g_t * DH), bf16),
            pltpu.VMEM((n_head, rows, n_s * DH), bf16),
            pltpu.VMEM((n_head, n_kv, rows, g_s * DH), bf16),
            pltpu.VMEM((n_t, DH, rows), bf16),
            pltpu.VMEM((HS, DH, rows), bf16),
            pltpu.VMEM((2, g_t * KVS, 2 * DH + 16, rows), bf16),
            pltpu.VMEM((2, n_t, rows, rows), bf16),
            pltpu.VMEM((n_t, 2 * DH + 16, rows), f32),
            pltpu.VMEM((n_t, 1, rows), f32),
            pltpu.VMEM((2, n_t, 1, rows), f32),
            pltpu.VMEM((n_s, 1, rows), f32),
            pltpu.VMEM((n_s, 1, rows), f32),
            pltpu.SMEM(pair_table.shape[::-1], jnp.int32),
            pltpu.SMEM((n_t,), jnp.int32),
            pltpu.VMEM((n_head * pad, rows), f32),
            pltpu.VMEM((max(n_head - 1, 1), pad, rows), f32),
            pltpu.VMEM((n_head, 1, 128), f32),
            pltpu.VMEM((n_rank, 1, 128), f32),
            pltpu.SemaphoreType.REGULAR,
            pltpu.SemaphoreType.REGULAR((2,)),
            dma((5,)),
            dma((n_kv, max(n_head - 1, 1))),
            dma((n_kv, max(n_head - 1, 1))),
            dma((3, max(n_head - 1, 1))),
            dma((3, max(n_head - 1, 1))),
            dma((max(n_head - 1, 1),)),
            dma((max(n_head - 1, 1),)),
            dma((n_kv, n_head + 2)),
            dma((n_kv, n_head + 2)),
            dma(()),
            dma(()),
        ],
        compiler_params=pltpu.CompilerParams(collective_id=0, has_side_effects=True),
    )(pair_table.T, teacher_query, teacher_key, student_query, student_key)
    kl, loss = pl.pallas_call(
        finish,
        out_shape=(
            jax.ShapeDtypeStruct((n_s, 1, rows), f32),
            jax.ShapeDtypeStruct((1, n_s), f32),
        ),
        in_specs=[pl.BlockSpec(memory_space=pltpu.VMEM)] * 2,
        out_specs=(
            pl.BlockSpec(memory_space=pltpu.VMEM),
            pl.BlockSpec(memory_space=pltpu.VMEM),
        ),
    )(pltpu.with_memory_space_constraint(kl, pltpu.VMEM), pltpu.with_memory_space_constraint(loss, pltpu.VMEM))
    return kl.reshape(1, n_s, rows), loss.reshape(n_s)


def solution(mesh):
    split = P("dp", "kv", "head")
    return jax.shard_map(
        per_device,
        mesh=mesh,
        in_specs=(split, split, split, split, P()),
        out_specs=(P("dp", "head", "kv"), P("head")),
        check_vma=False,
    )
```

```python
import functools
import math

import jax
import jax.numpy as jnp
from jax import lax
from jax.experimental import pallas as pl
from jax.experimental.pallas import tpu as pltpu
from jax.sharding import PartitionSpec as P

HT = 28
KVT = 4
DH = 128
HS = 14
KVS = 2

MESH = pl.DeviceIdType.MESH
LOWEST = -1e30


def nn(a, b):
    return jnp.dot(a, b, preferred_element_type=jnp.float32)


def flip(x):
    n = x.shape[1]
    eye = (
        lax.broadcasted_iota(jnp.int32, (n, n), 0) == lax.broadcasted_iota(jnp.int32, (n, n), 1)
    ).astype(jnp.bfloat16)
    out = lax.dot_general(eye, x, (((1,), (1,)), ((), ())), preferred_element_type=jnp.float32)
    return out.astype(jnp.bfloat16)


def kernel(
    n_dp, n_head, n_kv, rows, shared,
    table_hbm, tq_hbm, tk_hbm, sq_hbm, sk_hbm,
    kl_ref, loss_ref,
    tq, tk, sq, sk,
    tq_t, sq_t, key_t, weights, mixed, t_max, t_decay, s_max, s_sum,
    table, inverse, acc, acc_in, sums_out, sums,
    layer_sem, chain_sem, load_sem, key_send, key_recv, query_send, query_recv,
    back_send, back_recv, z_send, z_recv, sum_send, sum_recv,
):
    n_t, n_s = HT // n_head, HS // n_head
    g_t, g_s = KVT // n_head, KVS // n_head
    per_t, per_s = HT // KVT, HS // KVS
    dp, hd, kv = lax.axis_index("dp"), lax.axis_index("head"), lax.axis_index("kv")
    n_rank = n_dp * n_head * n_kv
    rank = (dp * n_head + hd) * n_kv + kv
    scale = 1.0 / math.sqrt(DH)
    rate = scale * math.log2(math.e)
    bf16 = jnp.bfloat16

    loads = [
        pltpu.make_async_copy(sk_hbm.at[0], sk.at[hd, kv], load_sem.at[0]),
        pltpu.make_async_copy(tk_hbm.at[0], tk.at[kv], load_sem.at[1]),
        pltpu.make_async_copy(sq_hbm.at[0], sq.at[hd], load_sem.at[2]),
        pltpu.make_async_copy(table_hbm, table, load_sem.at[3]),
        pltpu.make_async_copy(tq_hbm.at[0], tq, load_sem.at[4]),
    ]
    for load in loads:
        load.start()

    first, last = kv == 0, kv == n_kv - 1
    not_first, not_last = kv > 0, kv < n_kv - 1
    barrier = pltpu.get_barrier_semaphore()

    def greet(sem, **peer):
        pl.semaphore_signal(sem, inc=1, device_id=peer, device_id_type=MESH)

    @pl.when(not_first)
    def _():
        greet(barrier, kv=kv - 1)

    @pl.when(not_last)
    def _():
        greet(barrier, kv=kv + 1)

    for s in range(1, n_head):
        greet(barrier, head=(hd + s) % n_head)
    for s in range(1, n_dp):
        greet(barrier, dp=(dp + s) % n_dp)

    def column(step):
        return (hd + step) % n_head

    def across(step, src, dst, send, recv):
        return pltpu.make_async_remote_copy(
            src_ref=src, dst_ref=dst, send_sem=send, recv_sem=recv,
            device_id={"head": column(step)}, device_id_type=MESH,
        )

    def keys_over(block):
        return [
            across(
                s, sk.at[hd, block], sk.at[hd, block],
                key_send.at[block, s - 1], key_recv.at[block, s - 1],
            )
            for s in range(1, n_head)
        ]

    cuts = [0, n_s * 2 // 7, n_s * 5 // 7, n_s]
    n_group = len(cuts) - 1

    def queries_over(group):
        part = sq.at[hd, :, cuts[group] * DH:cuts[group + 1] * DH]
        return [
            across(s, part, part, query_send.at[group, s - 1], query_recv.at[group, s - 1])
            for s in range(1, n_head)
        ]

    def start(copies):
        for copy in copies:
            copy.start()

    half = rows // 2
    halves = (n_head, n_head + 1)

    def upward(block, piece):
        if piece < n_head:
            ref = sk.at[column(piece), block]
        else:
            ref = tk.at[block, pl.ds((piece - n_head) * half, half)]
        return pltpu.make_async_remote_copy(
            src_ref=ref, dst_ref=ref, send_sem=z_send.at[block, piece],
            recv_sem=z_recv.at[block, piece],
            device_id={"kv": jnp.minimum(kv + 1, n_kv - 1)}, device_id_type=MESH,
        )

    def launch(block, piece):
        @pl.when(not_last)
        def _():
            upward(block, piece).start()

    def land(block, piece):
        upward(block, piece).wait_recv()
        launch(block, piece)

    def receive_own(block):
        @pl.when(block >= shared)
        def _():
            land(block, 0)
            start(keys_over(block))

    def receive_teacher(block):
        for piece in halves:
            land(block, piece)

    def receive_student(block):
        @pl.when(block < shared)
        def _():
            land(block, 0)
            for s in range(1, n_head):
                land(block, s)

    loads[0].wait()
    pl.semaphore_wait(
        barrier, n_dp - 1 + n_head - 1 + not_first.astype(jnp.int32) + not_last.astype(jnp.int32)
    )
    start(keys_over(kv))

    @pl.when(kv < shared)
    def _():
        loads[1].wait()
        for piece in halves:
            launch(kv, piece)
        launch(kv, 0)

    @pl.when(kv >= shared)
    def _():
        launch(kv, 0)
        loads[1].wait()
        for piece in halves:
            launch(kv, piece)

    loads[2].wait()
    start(queries_over(0))

    @pl.when(not_last)
    def _():
        start(queries_over(1))
        start(queries_over(2))

    for s in range(1, n_head):
        greet(layer_sem, head=column(s))

    loads[3].wait()
    entries = [table[k % 2, k // 2] for k in range(HT)]
    for t in range(n_t):
        found = jnp.int32(0)
        for k in range(HT):
            found = jnp.where(entries[k] == hd * n_t + t, k // 2, found)
        inverse[t] = found

    loads[4].wait()
    for h in range(n_t):
        tq_t[h] = flip(tq[:, h * DH:(h + 1) * DH])
    for h in range(n_s):
        sq_t[hd * n_s + h] = flip(sq[hd, :, h * DH:(h + 1) * DH])
    key_t[:, :, 2 * DH:] = jnp.ones((2, g_t * KVS, 16, rows), bf16)
    mixed[...] = jnp.zeros(mixed.shape, jnp.float32)

    pl.semaphore_wait(layer_sem, n_head - 1)
    for way, inner in ((0, not_last), (1, not_first)):
        @pl.when(not_first & not_last)
        def _():
            pl.semaphore_wait(chain_sem.at[way], 1)

        @pl.when(inner)
        def _():
            greet(chain_sem.at[way], kv=kv + 1 - 2 * way)

    @pl.when(kv < shared)
    def _():
        for copy in keys_over(kv):
            copy.wait_recv()
        for s in range(1, n_head):
            launch(kv, s)

    @pl.when(not_last & not_first)
    def _():
        receive_own(kv - 1)
        receive_teacher(kv - 1)
        receive_student(kv - 1)

    visible = lax.broadcasted_iota(jnp.int32, (rows, rows), 0) <= lax.broadcasted_iota(
        jnp.int32, (rows, rows), 1
    )

    def weigh(logits, high, row, diagonal):
        if diagonal:
            logits = jnp.where(visible, logits, LOWEST)
        top = jnp.max(logits, axis=0, keepdims=True)
        if diagonal:
            decay = jnp.zeros_like(top)
        else:
            old = high[row]
            top = jnp.maximum(old, top)
            decay = jnp.exp2((old - top) * rate)
        high[row] = top
        return jnp.exp2((logits - top) * rate), decay

    def turn_student(c, block, slot):
        for j in range(g_s):
            flipped = flip(sk[c, block, :, j * DH:(j + 1) * DH])
            for g in range(g_t):
                key_t[slot, g * KVS + c * g_s + j, DH:2 * DH] = flipped

    def weigh_block(block, slot, diagonal):
        if not diagonal:
            @pl.when(last)
            def _():
                for piece in halves:
                    upward(block, piece).wait_recv()

        for h in range(n_t):
            g = h // per_t
            logits = nn(tk[block, :, g * DH:(g + 1) * DH], tq_t[h])
            weight, t_decay[slot, h] = weigh(logits, t_max, h, diagonal)
            weights[slot, h] = weight.astype(bf16)
        for g in range(g_t):
            flipped = flip(tk[block, :, g * DH:(g + 1) * DH])
            for j in range(KVS):
                key_t[slot, g * KVS + j, :DH] = flipped

        if not diagonal:
            @pl.when(last & (block < shared))
            def _():
                upward(block, 0).wait_recv()

        for h in range(n_s):
            g = h // per_s
            logits = nn(sk[hd, block, :, g * DH:(g + 1) * DH], sq_t[hd * n_s + h])
            weight, decay = weigh(logits, s_max, h, diagonal)
            part = jnp.sum(weight, axis=0, keepdims=True)
            s_sum[h] = part if diagonal else s_sum[h] * decay + part
        turn_student(hd, block, slot)

    def await_others(block):
        @pl.when((block < shared) & last & not_first & (block != kv))
        def _():
            for s in range(1, n_head):
                upward(block, s).wait_recv()

        @pl.when(block >= shared)
        def _():
            for copy in keys_over(block):
                copy.wait_recv()

    def turn_others(block, slot):
        for s in range(1, n_head):
            turn_student(column(s), block, slot)

    def mix(h, slot, blend):
        part = nn(key_t[slot, h // per_t * KVS + inverse[h] // per_s], weights[slot, h])
        return blend * t_decay[slot, h] + part

    def turn_queries(groups):
        for group in groups:
            for copy in queries_over(group):
                copy.wait_recv()
            for s in range(1, n_head):
                for h in range(cuts[group], cuts[group + 1]):
                    sq_t[column(s) * n_s + h] = flip(sq[column(s), :, h * DH:(h + 1) * DH])

    def after_own():
        @pl.when(last & not_first)
        def _():
            receive_own(kv - 1)

        @pl.when(last)
        def _():
            start(queries_over(1))

        @pl.when(last & first)
        def _():
            start(queries_over(2))

    weigh_block(kv, 0, True)
    after_own()

    def blend_before(s):
        await_others(kv - s + 1)
        turn_others(kv - s + 1, (s - 1) % 2)
        for h in range(n_t):
            mixed[h] = mix(h, (s - 1) % 2, mixed[h])

    def step(s, carry):
        block = kv - s

        @pl.when(not_last & (s < kv))
        def _():
            receive_own(block - 1)
            receive_teacher(block - 1)

        @pl.when(s < kv)
        def _():
            blend_before(s)

        @pl.when(not_last & (s < kv))
        def _():
            receive_student(block - 1)

        @pl.when(s == kv - 1)
        def _():
            turn_queries((0,))

        @pl.when((s == kv) & (s > 1))
        def _():
            turn_queries((1,))

        weigh_block(block, s % 2, False)

        @pl.when(last & (s < kv))
        def _():
            receive_own(block - 1)

        @pl.when(last & (s == 1))
        def _():
            start(queries_over(2))

        return carry

    lax.fori_loop(1, kv + 1, step, 0)

    @pl.when(kv <= 1)
    def _():
        turn_queries((0, 1))

    pad = acc.shape[0] // n_head
    place = lax.broadcasted_iota(jnp.int32, acc.shape, 0)
    lse = jnp.concatenate(
        [s_max[h] * scale + jnp.log(s_sum[h]) for h in range(n_s)]
        + [jnp.zeros((1, rows), jnp.float32)] * (pad - n_s),
        axis=0,
    )
    mine = jnp.where(place // pad == hd, 2.0 * jnp.concatenate([lse] * n_head, axis=0), 0.0)
    @pl.when(first)
    def _():
        key_t[1, :, :2 * DH] = jnp.zeros((g_t * KVS, 2 * DH, rows), bf16)
        weights[1] = jnp.zeros((n_t, rows, rows), bf16)
        t_decay[1] = jnp.zeros((n_t, 1, rows), jnp.float32)

    @pl.when(not_first)
    def _():
        await_others(1)
        turn_others(1, (kv - 1) % 2)

    await_others(0)
    turn_queries((2,))
    turn_others(0, kv % 2)
    total = jnp.zeros(acc.shape, jnp.float32)
    for h in range(n_t):
        partner = inverse[h]
        blend = mix(h, kv % 2, mix(h, (kv + 1) % 2, mixed[h]))
        own = blend[:DH] * tq_t[h].astype(jnp.float32)
        other = blend[DH:2 * DH] * sq_t[partner].astype(jnp.float32)
        mass = blend[2 * DH:2 * DH + 1]
        value = jnp.sum(own - other, axis=0, keepdims=True) * scale / mass
        value = value - (t_max[h] * scale + jnp.log(mass))
        row = (partner // n_s) * pad + partner % n_s
        total = total + jnp.where(place == row, value, 0.0)
    acc[...] = total

    returns = [
        across(
            s, acc.at[pl.ds(column(s) * pad, pad)], acc_in.at[s - 1],
            back_send.at[s - 1], back_recv.at[s - 1],
        )
        for s in range(1, n_head)
    ]
    start(returns)
    side = jnp.sum(total + mine, axis=1, keepdims=True)
    across_lanes = lax.broadcasted_iota(jnp.int32, (n_head * pad, 128), 1)
    down_rows = lax.broadcasted_iota(jnp.int32, (n_head * pad, 128), 0)
    for d in range(n_head):
        sums_out[d] = jnp.sum(
            jnp.where(down_rows == across_lanes + d * pad, side, 0.0), axis=0, keepdims=True
        )

    def share(d, h, k):
        return pltpu.make_async_remote_copy(
            src_ref=sums_out.at[h], dst_ref=sums.at[rank],
            send_sem=sum_send, recv_sem=sum_recv,
            device_id=(d, h, k), device_id_type=MESH,
        )

    def each_peer(act):
        def outer(k, carry):
            def middle(d, carry):
                for h in range(n_head):
                    @pl.when((d * n_head + h) * n_kv + k != rank)
                    def _():
                        act(d, h, k)
                return carry
            return lax.fori_loop(0, n_dp, middle, carry)
        lax.fori_loop(0, n_kv, outer, 0)

    for way, edge in ((0, last), (1, first)):
        @pl.when(edge)
        def _():
            pl.semaphore_wait(chain_sem.at[way], 1)

    each_peer(lambda d, h, k: share(d, h, k).start())
    sums[rank] = sums_out[hd]
    kl = acc[pl.ds(hd * pad, pad)] + 2.0 * lse
    for s in range(1, n_head):
        returns[s - 1].wait()
        kl = kl + acc_in[s - 1]
    for h in range(n_s):
        kl_ref[h] = kl[h:h + 1]

    for group in range(n_group):
        for copy in queries_over(group):
            copy.wait_send()

    def drain(block, carry):
        @pl.when((block >= shared) | (block == kv))
        def _():
            for copy in keys_over(block):
                copy.wait_send()

        @pl.when(not_last)
        def _():
            upward(block, 0).wait_send()
            for piece in halves:
                upward(block, piece).wait_send()

            @pl.when(block < shared)
            def _():
                for s in range(1, n_head):
                    upward(block, s).wait_send()
        return carry

    lax.fori_loop(0, kv + 1, drain, 0)

    others = sums.at[pl.ds(0, n_rank - 1)]
    pltpu.make_async_remote_copy(
        src_ref=others, dst_ref=others, send_sem=sum_send, recv_sem=sum_recv,
        device_id={"head": column(1)}, device_id_type=MESH,
    ).wait()
    line = jnp.sum(sums[...], axis=0)
    loss_ref[...] = line[:, :n_s] * (1.0 / (n_dp * rows * n_kv))


def finish(kl_in, loss_in, kl_ref, loss_ref):
    kl_ref[...] = kl_in[...]
    loss_ref[...] = loss_in[...]


def per_device(teacher_query, teacher_key, student_query, student_key, pair_table):
    n_dp, n_head, n_kv = lax.axis_size("dp"), lax.axis_size("head"), lax.axis_size("kv")
    seq_dev, rows, wide_t = teacher_query.shape
    assert seq_dev == 1
    n_t, n_s = HT // n_head, HS // n_head
    g_t, g_s = KVT // n_head, KVS // n_head
    n_rank = n_dp * n_head * n_kv
    pad = -(-n_s // 8) * 8
    key_t, key_s, query_s = g_t * DH, g_s * DH, n_s * DH
    spare = query_s + n_kv * key_s - (n_kv - 1) * (key_t + key_s)
    shared = min(max(round(spare / (2 * key_s * max(n_head - 1, 1))), 0), n_kv - 1)
    f32, bf16 = jnp.float32, jnp.bfloat16
    dma = pltpu.SemaphoreType.DMA
    kl, loss = pl.pallas_call(
        functools.partial(kernel, n_dp, n_head, n_kv, rows, shared),
        out_shape=(
            pltpu.VMEM((n_s, 1, rows), f32),
            pltpu.VMEM((1, n_s), f32),
        ),
        in_specs=[pl.BlockSpec(memory_space=pl.ANY)] * 5,
        out_specs=(
            pl.BlockSpec(memory_space=pltpu.VMEM),
            pl.BlockSpec(memory_space=pltpu.VMEM),
        ),
        scratch_shapes=[
            pltpu.VMEM((rows, wide_t), bf16),
            pltpu.VMEM((n_kv, rows, g_t * DH), bf16),
            pltpu.VMEM((n_head, rows, n_s * DH), bf16),
            pltpu.VMEM((n_head, n_kv, rows, g_s * DH), bf16),
            pltpu.VMEM((n_t, DH, rows), bf16),
            pltpu.VMEM((HS, DH, rows), bf16),
            pltpu.VMEM((2, g_t * KVS, 2 * DH + 16, rows), bf16),
            pltpu.VMEM((2, n_t, rows, rows), bf16),
            pltpu.VMEM((n_t, 2 * DH + 16, rows), f32),
            pltpu.VMEM((n_t, 1, rows), f32),
            pltpu.VMEM((2, n_t, 1, rows), f32),
            pltpu.VMEM((n_s, 1, rows), f32),
            pltpu.VMEM((n_s, 1, rows), f32),
            pltpu.SMEM(pair_table.shape[::-1], jnp.int32),
            pltpu.SMEM((n_t,), jnp.int32),
            pltpu.VMEM((n_head * pad, rows), f32),
            pltpu.VMEM((max(n_head - 1, 1), pad, rows), f32),
            pltpu.VMEM((n_head, 1, 128), f32),
            pltpu.VMEM((n_rank, 1, 128), f32),
            pltpu.SemaphoreType.REGULAR,
            pltpu.SemaphoreType.REGULAR((2,)),
            dma((5,)),
            dma((n_kv, max(n_head - 1, 1))),
            dma((n_kv, max(n_head - 1, 1))),
            dma((3, max(n_head - 1, 1))),
            dma((3, max(n_head - 1, 1))),
            dma((max(n_head - 1, 1),)),
            dma((max(n_head - 1, 1),)),
            dma((n_kv, n_head + 2)),
            dma((n_kv, n_head + 2)),
            dma(()),
            dma(()),
        ],
        compiler_params=pltpu.CompilerParams(collective_id=0, has_side_effects=True),
    )(pair_table.T, teacher_query, teacher_key, student_query, student_key)
    kl, loss = pl.pallas_call(
        finish,
        out_shape=(
            jax.ShapeDtypeStruct((n_s, 1, rows), f32),
            jax.ShapeDtypeStruct((1, n_s), f32),
        ),
        in_specs=[pl.BlockSpec(memory_space=pltpu.VMEM)] * 2,
        out_specs=(
            pl.BlockSpec(memory_space=pltpu.VMEM),
            pl.BlockSpec(memory_space=pltpu.VMEM),
        ),
    )(pltpu.with_memory_space_constraint(kl, pltpu.VMEM), pltpu.with_memory_space_constraint(loss, pltpu.VMEM))
    return kl.reshape(1, n_s, rows), loss.reshape(n_s)


def solution(mesh):
    split = P("dp", "kv", "head")
    return jax.shard_map(
        per_device,
        mesh=mesh,
        in_specs=(split, split, split, split, P()),
        out_specs=(P("dp", "head", "kv"), P("head")),
        check_vma=False,
    )
```

```python
import functools
import math

import jax
import jax.numpy as jnp
from jax import lax
from jax.experimental import pallas as pl
from jax.experimental.pallas import tpu as pltpu
from jax.sharding import PartitionSpec as P

HT = 28
KVT = 4
DH = 128
HS = 14
KVS = 2

MESH = pl.DeviceIdType.MESH
LOWEST = -1e30


def nn(a, b):
    return jnp.dot(a, b, preferred_element_type=jnp.float32)


def flip(x):
    n = x.shape[1]
    eye = (
        lax.broadcasted_iota(jnp.int32, (n, n), 0) == lax.broadcasted_iota(jnp.int32, (n, n), 1)
    ).astype(jnp.bfloat16)
    out = lax.dot_general(eye, x, (((1,), (1,)), ((), ())), preferred_element_type=jnp.float32)
    return out.astype(jnp.bfloat16)


def kernel(
    n_dp, n_head, n_kv, rows, shared,
    table_hbm, tq_hbm, tk_hbm, sq_hbm, sk_hbm,
    kl_ref, loss_ref,
    tq, tk, sq, sk,
    tq_t, sq_t, key_t, weights, mixed, t_max, t_decay, s_max, s_sum,
    table, inverse, acc, acc_in, sums_out, sums,
    layer_sem, chain_sem, load_sem, key_send, key_recv, query_send, query_recv,
    back_send, back_recv, z_send, z_recv, sum_send, sum_recv,
):
    n_t, n_s = HT // n_head, HS // n_head
    g_t, g_s = KVT // n_head, KVS // n_head
    per_t, per_s = HT // KVT, HS // KVS
    dp, hd, kv = lax.axis_index("dp"), lax.axis_index("head"), lax.axis_index("kv")
    n_rank = n_dp * n_head * n_kv
    rank = (dp * n_head + hd) * n_kv + kv
    scale = 1.0 / math.sqrt(DH)
    rate = scale * math.log2(math.e)
    bf16 = jnp.bfloat16

    loads = [
        pltpu.make_async_copy(sk_hbm.at[0], sk.at[hd, kv], load_sem.at[0]),
        pltpu.make_async_copy(tk_hbm.at[0], tk.at[kv], load_sem.at[1]),
        pltpu.make_async_copy(sq_hbm.at[0], sq.at[hd], load_sem.at[2]),
        pltpu.make_async_copy(table_hbm, table, load_sem.at[3]),
        pltpu.make_async_copy(tq_hbm.at[0], tq, load_sem.at[4]),
    ]
    for load in loads:
        load.start()

    first, last = kv == 0, kv == n_kv - 1
    not_first, not_last = kv > 0, kv < n_kv - 1
    barrier = pltpu.get_barrier_semaphore()

    def greet(sem, **peer):
        pl.semaphore_signal(sem, inc=1, device_id=peer, device_id_type=MESH)

    @pl.when(not_first)
    def _():
        greet(barrier, kv=kv - 1)

    @pl.when(not_last)
    def _():
        greet(barrier, kv=kv + 1)

    for s in range(1, n_head):
        greet(barrier, head=(hd + s) % n_head)
    for s in range(1, n_dp):
        greet(barrier, dp=(dp + s) % n_dp)

    def column(step):
        return (hd + step) % n_head

    def across(step, src, dst, send, recv):
        return pltpu.make_async_remote_copy(
            src_ref=src, dst_ref=dst, send_sem=send, recv_sem=recv,
            device_id={"head": column(step)}, device_id_type=MESH,
        )

    def keys_over(block):
        return [
            across(
                s, sk.at[hd, block], sk.at[hd, block],
                key_send.at[block, s - 1], key_recv.at[block, s - 1],
            )
            for s in range(1, n_head)
        ]

    cuts = [0, n_s * 2 // 7, n_s * 5 // 7, n_s]
    n_group = len(cuts) - 1

    def queries_over(group):
        part = sq.at[hd, :, cuts[group] * DH:cuts[group + 1] * DH]
        return [
            across(s, part, part, query_send.at[group, s - 1], query_recv.at[group, s - 1])
            for s in range(1, n_head)
        ]

    def start(copies):
        for copy in copies:
            copy.start()

    half = rows // 2
    halves = (n_head, n_head + 1)

    def upward(block, piece):
        if piece < n_head:
            ref = sk.at[column(piece), block]
        else:
            ref = tk.at[block, pl.ds((piece - n_head) * half, half)]
        return pltpu.make_async_remote_copy(
            src_ref=ref, dst_ref=ref, send_sem=z_send.at[block, piece],
            recv_sem=z_recv.at[block, piece],
            device_id={"kv": jnp.minimum(kv + 1, n_kv - 1)}, device_id_type=MESH,
        )

    def launch(block, piece):
        @pl.when(not_last)
        def _():
            upward(block, piece).start()

    def land(block, piece):
        upward(block, piece).wait_recv()
        launch(block, piece)

    def receive_own(block):
        @pl.when(block >= shared)
        def _():
            land(block, 0)
            start(keys_over(block))

    def receive_teacher(block):
        for piece in halves:
            land(block, piece)

    def receive_student(block):
        @pl.when(block < shared)
        def _():
            land(block, 0)
            for s in range(1, n_head):
                land(block, s)

    loads[0].wait()
    pl.semaphore_wait(
        barrier, n_dp - 1 + n_head - 1 + not_first.astype(jnp.int32) + not_last.astype(jnp.int32)
    )
    start(keys_over(kv))

    @pl.when(kv < shared)
    def _():
        loads[1].wait()
        for piece in halves:
            launch(kv, piece)
        launch(kv, 0)

    @pl.when(kv >= shared)
    def _():
        launch(kv, 0)
        loads[1].wait()
        for piece in halves:
            launch(kv, piece)

    loads[2].wait()
    start(queries_over(0))

    @pl.when(not_last)
    def _():
        start(queries_over(1))
        start(queries_over(2))

    for s in range(1, n_head):
        greet(layer_sem, head=column(s))

    loads[3].wait()
    entries = [table[k % 2, k // 2] for k in range(HT)]
    for t in range(n_t):
        found = jnp.int32(0)
        for k in range(HT):
            found = jnp.where(entries[k] == hd * n_t + t, k // 2, found)
        inverse[t] = found

    loads[4].wait()
    for h in range(n_t):
        tq_t[h] = flip(tq[:, h * DH:(h + 1) * DH])
    for h in range(n_s):
        sq_t[hd * n_s + h] = flip(sq[hd, :, h * DH:(h + 1) * DH])
    key_t[:, :, 2 * DH:] = jnp.ones((2, g_t * KVS, 16, rows), bf16)
    mixed[...] = jnp.zeros(mixed.shape, jnp.float32)

    pl.semaphore_wait(layer_sem, n_head - 1)
    for way, inner in ((0, not_last), (1, not_first)):
        @pl.when(not_first & not_last)
        def _():
            pl.semaphore_wait(chain_sem.at[way], 1)

        @pl.when(inner)
        def _():
            greet(chain_sem.at[way], kv=kv + 1 - 2 * way)

    @pl.when(kv < shared)
    def _():
        for copy in keys_over(kv):
            copy.wait_recv()
        for s in range(1, n_head):
            launch(kv, s)

    @pl.when(not_last & not_first)
    def _():
        receive_own(kv - 1)
        receive_teacher(kv - 1)
        receive_student(kv - 1)

    visible = lax.broadcasted_iota(jnp.int32, (rows, rows), 0) <= lax.broadcasted_iota(
        jnp.int32, (rows, rows), 1
    )

    def weigh(logits, high, row, diagonal):
        if diagonal:
            logits = jnp.where(visible, logits, LOWEST)
        top = jnp.max(logits, axis=0, keepdims=True)
        if diagonal:
            decay = jnp.zeros_like(top)
        else:
            old = high[row]
            top = jnp.maximum(old, top)
            decay = jnp.exp2((old - top) * rate)
        high[row] = top
        return jnp.exp2((logits - top) * rate), decay

    def turn_student(c, block, slot):
        for j in range(g_s):
            flipped = flip(sk[c, block, :, j * DH:(j + 1) * DH])
            for g in range(g_t):
                key_t[slot, g * KVS + c * g_s + j, DH:2 * DH] = flipped

    def weigh_block(block, slot, diagonal):
        if not diagonal:
            @pl.when(last)
            def _():
                for piece in halves:
                    upward(block, piece).wait_recv()

        for h in range(n_t):
            g = h // per_t
            logits = nn(tk[block, :, g * DH:(g + 1) * DH], tq_t[h])
            weight, t_decay[slot, h] = weigh(logits, t_max, h, diagonal)
            weights[slot, h] = weight.astype(bf16)
        for g in range(g_t):
            flipped = flip(tk[block, :, g * DH:(g + 1) * DH])
            for j in range(KVS):
                key_t[slot, g * KVS + j, :DH] = flipped

        if not diagonal:
            @pl.when(last & (block < shared))
            def _():
                upward(block, 0).wait_recv()

        for h in range(n_s):
            g = h // per_s
            logits = nn(sk[hd, block, :, g * DH:(g + 1) * DH], sq_t[hd * n_s + h])
            weight, decay = weigh(logits, s_max, h, diagonal)
            part = jnp.sum(weight, axis=0, keepdims=True)
            s_sum[h] = part if diagonal else s_sum[h] * decay + part
        turn_student(hd, block, slot)

    def await_others(block):
        @pl.when((block < shared) & last & not_first & (block != kv))
        def _():
            for s in range(1, n_head):
                upward(block, s).wait_recv()

        @pl.when(block >= shared)
        def _():
            for copy in keys_over(block):
                copy.wait_recv()

    def turn_others(block, slot):
        for s in range(1, n_head):
            turn_student(column(s), block, slot)

    def mix(h, slot, blend):
        part = nn(key_t[slot, h // per_t * KVS + inverse[h] // per_s], weights[slot, h])
        return blend * t_decay[slot, h] + part

    def turn_queries(groups):
        for group in groups:
            for copy in queries_over(group):
                copy.wait_recv()
            for s in range(1, n_head):
                for h in range(cuts[group], cuts[group + 1]):
                    sq_t[column(s) * n_s + h] = flip(sq[column(s), :, h * DH:(h + 1) * DH])

    def after_own():
        @pl.when(last & not_first)
        def _():
            receive_own(kv - 1)

        @pl.when(last)
        def _():
            start(queries_over(1))

        @pl.when(last & first)
        def _():
            start(queries_over(2))

    weigh_block(kv, 0, True)
    after_own()

    def blend_before(s):
        await_others(kv - s + 1)
        turn_others(kv - s + 1, (s - 1) % 2)
        for h in range(n_t):
            mixed[h] = mix(h, (s - 1) % 2, mixed[h])

    def step(s, carry):
        block = kv - s

        @pl.when(not_last & (s < kv))
        def _():
            receive_own(block - 1)
            receive_teacher(block - 1)

        @pl.when(s < kv)
        def _():
            blend_before(s)

        @pl.when(not_last & (s < kv))
        def _():
            receive_student(block - 1)

        @pl.when(s == kv - 1)
        def _():
            turn_queries((0,))

        @pl.when((s == kv) & (s > 1))
        def _():
            turn_queries((1,))

        weigh_block(block, s % 2, False)

        @pl.when(last & (s < kv))
        def _():
            receive_own(block - 1)

        @pl.when(last & (s == 1))
        def _():
            start(queries_over(2))

        return carry

    lax.fori_loop(1, kv + 1, step, 0)

    @pl.when(kv <= 1)
    def _():
        turn_queries((0, 1))

    pad = acc.shape[0] // n_head
    place = lax.broadcasted_iota(jnp.int32, acc.shape, 0)
    lse = jnp.concatenate(
        [s_max[h] * scale + jnp.log(s_sum[h]) for h in range(n_s)]
        + [jnp.zeros((1, rows), jnp.float32)] * (pad - n_s),
        axis=0,
    )
    mine = jnp.where(place // pad == hd, 2.0 * jnp.concatenate([lse] * n_head, axis=0), 0.0)
    @pl.when(first)
    def _():
        key_t[1, :, :2 * DH] = jnp.zeros((g_t * KVS, 2 * DH, rows), bf16)
        weights[1] = jnp.zeros((n_t, rows, rows), bf16)
        t_decay[1] = jnp.zeros((n_t, 1, rows), jnp.float32)

    @pl.when(not_first)
    def _():
        await_others(1)
        turn_others(1, (kv - 1) % 2)

    for way, edge in ((0, last), (1, first)):
        @pl.when(edge)
        def _():
            pl.semaphore_wait(chain_sem.at[way], 1)

    await_others(0)
    turn_queries((2,))
    turn_others(0, kv % 2)
    total = jnp.zeros(acc.shape, jnp.float32)
    for h in range(n_t):
        partner = inverse[h]
        blend = mix(h, kv % 2, mix(h, (kv + 1) % 2, mixed[h]))
        own = blend[:DH] * tq_t[h].astype(jnp.float32)
        other = blend[DH:2 * DH] * sq_t[partner].astype(jnp.float32)
        mass = blend[2 * DH:2 * DH + 1]
        value = jnp.sum(own - other, axis=0, keepdims=True) * scale / mass
        value = value - (t_max[h] * scale + jnp.log(mass))
        row = (partner // n_s) * pad + partner % n_s
        total = total + jnp.where(place == row, value, 0.0)
    acc[...] = total

    returns = [
        across(
            s, acc.at[pl.ds(column(s) * pad, pad)], acc_in.at[s - 1],
            back_send.at[s - 1], back_recv.at[s - 1],
        )
        for s in range(1, n_head)
    ]
    side = jnp.sum(total + mine, axis=1, keepdims=True)
    across_lanes = lax.broadcasted_iota(jnp.int32, (n_head * pad, 128), 1)
    down_rows = lax.broadcasted_iota(jnp.int32, (n_head * pad, 128), 0)
    for d in range(n_head):
        sums_out[d] = jnp.sum(
            jnp.where(down_rows == across_lanes + d * pad, side, 0.0), axis=0, keepdims=True
        )

    def share(d, h, k):
        return pltpu.make_async_remote_copy(
            src_ref=sums_out.at[h], dst_ref=sums.at[rank],
            send_sem=sum_send, recv_sem=sum_recv,
            device_id=(d, h, k), device_id_type=MESH,
        )

    def each_peer(act):
        def outer(k, carry):
            def middle(d, carry):
                for h in range(n_head):
                    @pl.when((d * n_head + h) * n_kv + k != rank)
                    def _():
                        act(d, h, k)
                return carry
            return lax.fori_loop(0, n_dp, middle, carry)
        lax.fori_loop(0, n_kv, outer, 0)

    each_peer(lambda d, h, k: share(d, h, k).start())
    start(returns)
    sums[rank] = sums_out[hd]
    kl = acc[pl.ds(hd * pad, pad)] + 2.0 * lse
    for s in range(1, n_head):
        returns[s - 1].wait()
        kl = kl + acc_in[s - 1]
    for h in range(n_s):
        kl_ref[h] = kl[h:h + 1]

    for group in range(n_group):
        for copy in queries_over(group):
            copy.wait_send()

    def drain(block, carry):
        @pl.when((block >= shared) | (block == kv))
        def _():
            for copy in keys_over(block):
                copy.wait_send()

        @pl.when(not_last)
        def _():
            upward(block, 0).wait_send()
            for piece in halves:
                upward(block, piece).wait_send()

            @pl.when(block < shared)
            def _():
                for s in range(1, n_head):
                    upward(block, s).wait_send()
        return carry

    lax.fori_loop(0, kv + 1, drain, 0)

    others = sums.at[pl.ds(0, n_rank - 1)]
    pltpu.make_async_remote_copy(
        src_ref=others, dst_ref=others, send_sem=sum_send, recv_sem=sum_recv,
        device_id={"head": column(1)}, device_id_type=MESH,
    ).wait()
    line = jnp.sum(sums[...], axis=0)
    loss_ref[...] = line[:, :n_s] * (1.0 / (n_dp * rows * n_kv))


def finish(kl_in, loss_in, kl_ref, loss_ref):
    kl_ref[...] = kl_in[...]
    loss_ref[...] = loss_in[...]


def per_device(teacher_query, teacher_key, student_query, student_key, pair_table):
    n_dp, n_head, n_kv = lax.axis_size("dp"), lax.axis_size("head"), lax.axis_size("kv")
    seq_dev, rows, wide_t = teacher_query.shape
    assert seq_dev == 1
    n_t, n_s = HT // n_head, HS // n_head
    g_t, g_s = KVT // n_head, KVS // n_head
    n_rank = n_dp * n_head * n_kv
    pad = -(-n_s // 8) * 8
    key_t, key_s, query_s = g_t * DH, g_s * DH, n_s * DH
    spare = query_s + n_kv * key_s - (n_kv - 1) * (key_t + key_s)
    shared = min(max(round(spare / (2 * key_s * max(n_head - 1, 1))), 0), n_kv - 1)
    f32, bf16 = jnp.float32, jnp.bfloat16
    dma = pltpu.SemaphoreType.DMA
    kl, loss = pl.pallas_call(
        functools.partial(kernel, n_dp, n_head, n_kv, rows, shared),
        out_shape=(
            pltpu.VMEM((n_s, 1, rows), f32),
            pltpu.VMEM((1, n_s), f32),
        ),
        in_specs=[pl.BlockSpec(memory_space=pl.ANY)] * 5,
        out_specs=(
            pl.BlockSpec(memory_space=pltpu.VMEM),
            pl.BlockSpec(memory_space=pltpu.VMEM),
        ),
        scratch_shapes=[
            pltpu.VMEM((rows, wide_t), bf16),
            pltpu.VMEM((n_kv, rows, g_t * DH), bf16),
            pltpu.VMEM((n_head, rows, n_s * DH), bf16),
            pltpu.VMEM((n_head, n_kv, rows, g_s * DH), bf16),
            pltpu.VMEM((n_t, DH, rows), bf16),
            pltpu.VMEM((HS, DH, rows), bf16),
            pltpu.VMEM((2, g_t * KVS, 2 * DH + 16, rows), bf16),
            pltpu.VMEM((2, n_t, rows, rows), bf16),
            pltpu.VMEM((n_t, 2 * DH + 16, rows), f32),
            pltpu.VMEM((n_t, 1, rows), f32),
            pltpu.VMEM((2, n_t, 1, rows), f32),
            pltpu.VMEM((n_s, 1, rows), f32),
            pltpu.VMEM((n_s, 1, rows), f32),
            pltpu.SMEM(pair_table.shape[::-1], jnp.int32),
            pltpu.SMEM((n_t,), jnp.int32),
            pltpu.VMEM((n_head * pad, rows), f32),
            pltpu.VMEM((max(n_head - 1, 1), pad, rows), f32),
            pltpu.VMEM((n_head, 1, 128), f32),
            pltpu.VMEM((n_rank, 1, 128), f32),
            pltpu.SemaphoreType.REGULAR,
            pltpu.SemaphoreType.REGULAR((2,)),
            dma((5,)),
            dma((n_kv, max(n_head - 1, 1))),
            dma((n_kv, max(n_head - 1, 1))),
            dma((3, max(n_head - 1, 1))),
            dma((3, max(n_head - 1, 1))),
            dma((max(n_head - 1, 1),)),
            dma((max(n_head - 1, 1),)),
            dma((n_kv, n_head + 2)),
            dma((n_kv, n_head + 2)),
            dma(()),
            dma(()),
        ],
        compiler_params=pltpu.CompilerParams(collective_id=0, has_side_effects=True),
    )(pair_table.T, teacher_query, teacher_key, student_query, student_key)
    kl, loss = pl.pallas_call(
        finish,
        out_shape=(
            jax.ShapeDtypeStruct((n_s, 1, rows), f32),
            jax.ShapeDtypeStruct((1, n_s), f32),
        ),
        in_specs=[pl.BlockSpec(memory_space=pltpu.VMEM)] * 2,
        out_specs=(
            pl.BlockSpec(memory_space=pltpu.VMEM),
            pl.BlockSpec(memory_space=pltpu.VMEM),
        ),
    )(pltpu.with_memory_space_constraint(kl, pltpu.VMEM), pltpu.with_memory_space_constraint(loss, pltpu.VMEM))
    return kl.reshape(1, n_s, rows), loss.reshape(n_s)


def solution(mesh):
    split = P("dp", "kv", "head")
    return jax.shard_map(
        per_device,
        mesh=mesh,
        in_specs=(split, split, split, split, P()),
        out_specs=(P("dp", "head", "kv"), P("head")),
        check_vma=False,
    )
```
